8 devices in a mesh: dp: 2 (over z, y), tp: 4 (over x, core).
Axes of the slice: x: 2, y: 2, z: 1, core: 2. Of those that a mesh axis runs over, the one named last changes fastest.
Arguments:
- doc_hidden: bfloat16 [64, 16, 2048], P(('dp', 'tp')), parts along dimension 0
- doc_mask: int32 [64, 16], P(('dp', 'tp')), parts along dimension 0
- query_ids: int32 [64, 64], P(('dp', 'tp')), parts along dimension 0
- positive: int32 [64], P(('dp', 'tp')), parts along dimension 0
- tok_weight: float32 [32000], P('tp')
- w_head: bfloat16 [2048, 32000], P(None, 'tp')
- b_head: float32 [32000], P('tp')
Outputs:
- output 1: float32 [2], P('dp'), parts along dimension 0
- output 2: bfloat16 [4096, 32000], P('dp', 'tp'), parts along dimension 0
- output 3: float32 [64000], P(('dp', 'tp')), parts along dimension 0
- output 4: bfloat16 [64, 16, 2048], P(('dp', 'tp')), parts along dimension 0
There are 2 independent parts. The reference program is written for one: setup_inputs(seed, part) draws one part's arguments, and reference() takes and returns one part's arrays. A program takes and returns all parts, laid end to end along the dimension named above; an argument that names none is the same for every part.
All inputs are finite; a program needn't handle non-finite values.
Results may differ from the reference program's by a relative error of at most 0.001.
Values are sent between devices in bfloat16 or wider.
A program may use at most 1 GiB of HBM per device.

```python
import math
import jax
import jax.numpy as jnp
from jax import lax

HIDDEN = 2048
VOCAB = 32000
BATCH_DEV = 8
DOC_LEN = 16
QUERY_LEN = 64
GROUP_SIZE = 4
NUM_DOCS = BATCH_DEV * GROUP_SIZE
REG_COEF = 32.0


def setup_inputs(seed: int = 0, part: int = 0) -> dict:
    base_key = jax.random.key(seed)
    part_keys = jax.random.split(jax.random.fold_in(base_key, part), 6)
    shared_keys = jax.random.split(jax.random.key(seed + 1), 3)
    doc_hidden = jax.random.normal(part_keys[0], (NUM_DOCS, DOC_LEN, HIDDEN), jnp.float32)
    lengths = jax.random.randint(part_keys[1], (NUM_DOCS,), DOC_LEN - DOC_LEN // 4, DOC_LEN + 1)
    lengths = lengths.at[0].set(DOC_LEN)
    doc_mask = (jnp.arange(DOC_LEN)[None, :] < lengths[:, None]).astype(jnp.int32)
    hot_pick = jax.random.randint(part_keys[2], (NUM_DOCS, QUERY_LEN), 0, 2)
    hot_ids = jax.random.randint(part_keys[3], (NUM_DOCS, QUERY_LEN), 0, VOCAB // 4)
    any_ids = jax.random.randint(part_keys[4], (NUM_DOCS, QUERY_LEN), 0, VOCAB)
    query_ids = jnp.where(hot_pick == 0, hot_ids, any_ids).astype(jnp.int32)
    query_ids = query_ids.at[0, 0].set(0).at[0, 1].set(VOCAB - 1)
    positive = jax.random.permutation(part_keys[5], NUM_DOCS).astype(jnp.int32)
    w_head = jax.random.normal(shared_keys[0], (HIDDEN, VOCAB), jnp.float32) * HIDDEN ** -0.5
    b_head = -0.5 + 0.5 * jax.random.normal(shared_keys[1], (VOCAB,), jnp.float32)
    tok_weight = (0.5 + jax.random.uniform(shared_keys[2], (VOCAB,), jnp.float32)) * (2.0 / math.sqrt(QUERY_LEN * DOC_LEN))
    return {
        'doc_hidden': doc_hidden.astype(jnp.bfloat16),
        'doc_mask': doc_mask,
        'query_ids': query_ids,
        'positive': positive,
        'tok_weight': tok_weight,
        'w_head': w_head.astype(jnp.bfloat16),
        'b_head': b_head,
    }


def reference(doc_hidden, doc_mask, query_ids, positive, tok_weight, w_head, b_head):
    num_docs = doc_hidden.shape[0]
    num_queries = query_ids.shape[0]
    reg_weight = REG_COEF / (VOCAB * DOC_LEN * DOC_LEN)

    def doc_logits(hidden_doc):
        return jnp.dot(hidden_doc, w_head, preferred_element_type=jnp.float32) + b_head

    def doc_forward(doc_pair):
        hidden_doc, mask_doc = doc_pair
        sparse_act = jnp.log1p(jnp.maximum(doc_logits(hidden_doc), 0.0))
        return jnp.sum(sparse_act * mask_doc[:, None].astype(jnp.float32), axis=0)

    doc_rep = lax.map(doc_forward, (doc_hidden, doc_mask))
    query_rows = jnp.broadcast_to(jnp.arange(num_queries)[:, None], query_ids.shape)
    counts = jnp.zeros((num_queries, VOCAB), jnp.float32).at[query_rows, query_ids].add(1.0)
    query_rep = counts * tok_weight[None, :]
    scores = jnp.dot(query_rep, doc_rep.T, preferred_element_type=jnp.float32)
    onehot = (positive[:, None] == jnp.arange(num_docs)[None, :]).astype(jnp.float32)
    log_norm = jax.nn.logsumexp(scores, axis=1)
    col_mean = jnp.mean(doc_rep, axis=0)
    total_loss = jnp.mean(log_norm - jnp.sum(scores * onehot, axis=1)) + reg_weight * jnp.sum(col_mean * col_mean)
    d_scores = (jax.nn.softmax(scores, axis=1) - onehot) / num_queries
    d_rep = jnp.dot(d_scores.T, query_rep, preferred_element_type=jnp.float32) + (2.0 * reg_weight / num_docs) * col_mean[None, :]

    def doc_backward(acc_pair, doc_triple):
        dw_acc, db_acc = acc_pair
        hidden_doc, mask_doc, d_rep_doc = doc_triple
        logits = doc_logits(hidden_doc)
        relu_gate = jnp.where(logits > 0.0, 1.0 / (1.0 + jnp.maximum(logits, 0.0)), 0.0)
        d_logits = d_rep_doc[None, :] * mask_doc[:, None].astype(jnp.float32) * relu_gate
        d_low = d_logits.astype(jnp.bfloat16)
        dw_acc = dw_acc + jnp.dot(hidden_doc.T, d_low, preferred_element_type=jnp.float32)
        db_acc = db_acc + jnp.sum(d_logits, axis=0)
        hid_grad = jnp.dot(d_low, w_head.T, preferred_element_type=jnp.float32).astype(jnp.bfloat16)
        return (dw_acc, db_acc), hid_grad

    zero_acc = (jnp.zeros((HIDDEN, VOCAB), jnp.float32), jnp.zeros((VOCAB,), jnp.float32))
    (dw_sum, db_sum), d_hidden = lax.scan(doc_backward, zero_acc, (doc_hidden, doc_mask, d_rep))
    return total_loss.reshape(1), dw_sum.astype(jnp.bfloat16), db_sum, d_hidden
```

```python
import functools

import jax
import jax.numpy as jnp
from jax import lax
from jax.experimental import pallas as pl
from jax.experimental.pallas import tpu as pltpu
from jax.sharding import PartitionSpec as P

REG_COEF = 32.0
MESH = pl.DeviceIdType.MESH
F32 = jnp.float32
BF16 = jnp.bfloat16
VT = 512
LANES = 128
HALF = 256
ROWS = 128
SUB = 64
CHUNKS = 4
QUERIES = 32
NT_DIMS = (((1,), (1,)), ((), ()))
TN_DIMS = (((0,), (0,)), ((), ()))


def dot(a, b):
    return jnp.dot(a, b, preferred_element_type=F32)


def dot_nt(a, b):
    return lax.dot_general(a, b, NT_DIMS, preferred_element_type=F32)


def dot_tn(a, b):
    return lax.dot_general(a, b, TN_DIMS, preferred_element_type=F32)


def iota(shape, axis):
    return lax.broadcasted_iota(jnp.int32, shape, axis)


def one_hot(cond):
    return jnp.where(cond, 1.0, 0.0).astype(BF16)


def split3(x):
    hi = x.astype(BF16)
    rest = x - hi.astype(F32)
    mid = rest.astype(BF16)
    low = (rest - mid.astype(F32)).astype(BF16)
    return hi, mid, low


def log1p_pos(y):
    return jnp.where(y < 5e-4, y * (1.0 - 0.5 * y), jnp.log(1.0 + y))


def head_kernel(
    reg_weight,
    hid_ref, ids_ref, mask_ref, pos_ref, qw_hbm, bias_hbm, w_hbm,
    loss_ref, db_hbm, gt_hbm, hb_hbm, send_hbm, mine_hbm, part_hbm,
    wv, ybuf, hb, land, raw_a, raw_b, g_a, g_b, acc1, acc2, recv1,
    counts, bm, qw_ref, bias_ref, db_ref, mask_row, ids_all, mask_all, pos_all, s_acc, reg_acc, inbox, ds6,
    w_sem, hid_send, hid_recv, fwd_send, fwd_recv, pk_send, pk_recv, s_send, s_recv, acc_send, acc_recv, out_sem, g_sem,
):
    vocab = wv.shape[0]
    hidden = wv.shape[1]
    full = vocab // VT
    tail = vocab - full * VT
    me = lax.axis_index("tp")
    partner = me + 1 - 2 * lax.rem(me, 2)
    other = lax.rem(me + 2, 4)
    diag = lax.rem(partner + 2, 4)
    slots = (me, partner, other, diag)

    def remote(src, dst, ssem, rsem, dev):
        return pltpu.make_async_remote_copy(src, dst, ssem, rsem, device_id={"tp": dev}, device_id_type=MESH)

    def at(t, off=0, size=VT):
        if isinstance(t, int):
            return pl.ds(t * VT + off, size)
        return pl.ds(pl.multiple_of(t * VT + off, SUB), size)

    def cols(t, off=0, size=VT):
        if isinstance(t, int):
            return pl.ds(t * VT + off, size)
        return pl.ds(pl.multiple_of(t * VT + off, LANES), size)

    def w_copy(t, size=VT):
        return pltpu.make_async_copy(w_hbm.at[at(t, 0, size)], wv.at[at(t, 0, size)], w_sem.at[t])

    rows_in = [
        pltpu.make_async_copy(qw_hbm, qw_ref.at[0], out_sem.at[0]),
        pltpu.make_async_copy(bias_hbm, bias_ref.at[0], out_sem.at[1]),
    ]
    for c in rows_in:
        c.start()
    ahead = 6
    for t in range(ahead):
        w_copy(t).start()

    barrier = pltpu.get_barrier_semaphore()
    for peer in slots[1:]:
        pl.semaphore_signal(barrier, inc=1, device_id={"tp": peer}, device_id_type=MESH)
    pl.semaphore_wait(barrier, 3)

    pk_copies = []
    for k in range(3):
        for i, (src, dst) in enumerate(((ids_ref, ids_all), (mask_ref, mask_all), (pos_ref, pos_all))):
            pk_copies.append(remote(src, dst.at[me], pk_send.at[3 * k + i], pk_recv.at[3 * k + i], slots[k + 1]))
    for c in pk_copies:
        c.start()
    near = remote(hid_ref, land.at[0], hid_send.at[CHUNKS], hid_recv.at[CHUNKS], partner)
    near.start()
    step = ROWS // CHUNKS
    far, relay = [], []
    for k in range(CHUNKS):
        part = pl.ds(k * step, step)
        far.append(remote(hid_ref.at[part], land.at[1, part], hid_send.at[k], hid_recv.at[k], other))
        relay.append(remote(land.at[1, part], land.at[2, part], fwd_send.at[k], fwd_recv.at[k], partner))
    for c in far:
        c.start()

    ones = jnp.ones((16, LANES), BF16)
    sub16 = iota((16, VT), 0)

    def bias_columns(t, size):
        parts = [p.astype(F32) for p in split3(bias_ref[:, cols(t, 0, size)])]
        stack = jnp.zeros((16, size), F32)
        for k in range(3):
            stack = jnp.where(sub16[:, :size] == k, parts[k], stack)
        bm[at(t, 0, size)] = dot_tn(stack.astype(BF16), ones)

    def bias_body(t, carry):
        bias_columns(t, VT)
        return carry

    for c in rows_in:
        c.wait()
    lax.fori_loop(0, full, bias_body, 0)
    bias_columns(full, tail)
    ids_all[me] = ids_ref[...]
    mask_all[me] = mask_ref[...]
    pos_all[me] = pos_ref[...]
    for c in pk_copies:
        c.wait_recv()

    lane8 = iota((8, LANES), 1)
    for h in range(2):
        total = None
        for k in range(2):
            mask = mask_all[slots[2 * h + k]].astype(F32).astype(BF16)
            spread = dot(mask, one_hot((iota((16, LANES), 1) >> 4) + 8 == iota((16, LANES), 0)))
            piece = jnp.sum(jnp.where((lane8 & 15) == iota((8, LANES), 0) + 8 * k, spread, 0.0), axis=0, keepdims=True)
            total = piece if total is None else total + piece
        mask_row[h] = jnp.broadcast_to(total, (8, LANES))

    ids = jnp.concatenate([ids_all[g] for g in range(4)], axis=0)
    raw_a[pl.ds(0, LANES), pl.ds(0, LANES)] = jnp.zeros((LANES, LANES), F32)
    raw_a[pl.ds(0, QUERIES), pl.ds(0, 64)] = ids.astype(F32)
    ids_t = jnp.transpose(raw_a[pl.ds(0, LANES), pl.ds(0, LANES)])
    high = (ids - me * vocab) >> 7
    low = (ids_t.astype(jnp.int32) - me * vocab) & 127
    for q in range(QUERIES):
        hot_hi = one_hot(iota((64, 64), 0) == high[q:q + 1])
        hot_lo = one_hot(iota((64, LANES), 1) == low[:64, q:q + 1])
        counts[pl.ds(q, 64, QUERIES), :] = dot(hot_hi, hot_lo)
    s_acc[...] = jnp.zeros_like(s_acc)
    reg_acc[...] = jnp.zeros_like(reg_acc)

    def place(half, sources):
        r, k = iota((HALF, ROWS), 0), iota((HALF, ROWS), 1)
        pick = [one_hot((k == (r & 7) * 16 + (r >> 4)) & (((r >> 3) & 1) == s)) for s in range(2)]
        for c in range(hidden // VT):
            block = pl.ds(c * VT, VT)
            mixed = dot(pick[0], sources[0][:, block]) + dot(pick[1], sources[1][:, block])
            hb[half, :, block] = mixed.astype(BF16)

    near.wait_recv()
    place(0, (hid_ref, land.at[0]))

    def query_rep(t, off, size):
        out = []
        for c in range(-(-size // LANES)):
            width = min(LANES, size - c * LANES)
            block = t * (VT // LANES) + off // LANES + c
            start = block * QUERIES
            if not isinstance(t, int):
                start = pl.multiple_of(start, QUERIES)
            cnt = counts[pl.ds(start, QUERIES)]
            out.append(cnt[:, :width] * qw_ref[:, cols(t, off + c * LANES, width)])
        return jnp.concatenate(out, axis=1) if len(out) > 1 else out[0]

    def mm(t, half, buf, size=VT):
        buf[pl.ds(0, size)] = dot_nt(wv[at(t, 0, size)], hb[half])

    lane_sub = iota((SUB, LANES), 1)

    def ep(t, half, buf, size=VT):
        mask = mask_row[half, 0:1]
        for r in range(size // SUB):
            rows = pl.ds(r * SUB, SUB)
            here = at(t, r * SUB, SUB)
            col = bm[here]
            bias = col if half == 0 else jnp.broadcast_to(col[:, 0:1], (SUB, LANES))
            acc = None
            for b in range(2):
                y = jnp.maximum(buf[rows, pl.ds(b * LANES, LANES)] + bias, 0.0)
                if b == 1:
                    y = y * mask
                ybuf[here, pl.ds(half * HALF + b * LANES, LANES)] = y
                act = log1p_pos(y)
                acc = act if acc is None else acc + act
            buf[rows, pl.ds(0, LANES)] = acc
            total = jnp.sum(acc, axis=1, keepdims=True)
            if half == 0:
                bm[here] = jnp.where(lane_sub < 64, col, total)
            else:
                mean = jnp.broadcast_to((total + col[:, 64:65]) * (1.0 / 32.0), (SUB, LANES))
                bm[here] = mean
                square = mean * mean
                reg_acc[...] += jnp.sum(square.reshape(SUB // 8, 8, LANES), axis=0)
        for off in range(0, size, HALF):
            depth = min(HALF, size - off)
            rq = split3(query_rep(t, off, depth))
            act = split3(buf[pl.ds(off, depth), pl.ds(0, LANES)])
            s_acc[half] += dot(jnp.concatenate(rq, axis=0), act[0])
            s_acc[half, pl.ds(0, 64)] += dot(jnp.concatenate(rq[:2], axis=0), act[1])
            s_acc[half, pl.ds(0, 32)] += dot(rq[0], act[2])

    def forward(half, tick):
        first = half == 0
        if first:
            w_copy(0).wait()
        mm(0, half, raw_a)

        def body(i, carry):
            t = 2 * i
            if first:
                for u in range(2):
                    @pl.when(t + u + ahead < full)
                    def _():
                        w_copy(t + u + ahead).start()
                @pl.when(i == (full - ahead) // 2)
                def _():
                    w_copy(full, tail).start()
                w_copy(t + 1).wait()
            mm(t + 1, half, raw_b)
            ep(t, half, raw_a)
            if first:
                w_copy(t + 2).wait()
            mm(t + 2, half, raw_a)
            ep(t + 1, half, raw_b)
            tick(i)
            return carry

        lax.fori_loop(0, (full - 1) // 2, body, 0)
        if first:
            w_copy(full, tail).wait()
        mm(full, half, raw_b, tail)
        ep(full - 1, half, raw_a)
        ep(full, half, raw_b, tail)

    def relay_tick(i):
        for k, when in enumerate((0, 2, 4)):
            @pl.when(i == when)
            def _():
                far[k].wait_recv()
                relay[k].start()

    forward(0, relay_tick)
    far[CHUNKS - 1].wait_recv()
    relay[CHUNKS - 1].start()
    for c in relay:
        c.wait_recv()
    place(1, (land.at[1], land.at[2]))
    hb_out = pltpu.make_async_copy(hb, hb_hbm, out_sem.at[3])
    hb_out.start()
    forward(1, lambda i: None)

    def doc_lane(half):
        k = iota((LANES, LANES), 0)
        owner = jnp.where(((k >> 3) & 1) == 0, slots[2 * half], slots[2 * half + 1])
        return one_hot(iota((LANES, LANES), 1) == owner * 8 + (k & 7))

    scores = None
    for h in range(2):
        mine = s_acc[h, pl.ds(0, 32)] + s_acc[h, pl.ds(32, 32)] + s_acc[h, pl.ds(64, 32)]
        moved = dot(jnp.concatenate(split3(mine), axis=0), doc_lane(h))
        moved = moved[0:32] + moved[32:64] + moved[64:96]
        scores = moved if scores is None else scores + moved
    inbox[me, pl.ds(0, 32)] = scores
    inbox[me, pl.ds(32, 8)] = jnp.broadcast_to(jnp.sum(reg_acc[...], axis=0, keepdims=True), (8, LANES))
    s_copies = [remote(inbox.at[me], inbox.at[me], s_send.at[k], s_recv.at[k], slots[k + 1]) for k in range(3)]
    for c in s_copies:
        c.start()
    for c in s_copies:
        c.wait_recv()
    st = inbox[0] + inbox[1] + inbox[2] + inbox[3]
    lane = iota((32, LANES), 1)
    live = lane < 32
    score = jnp.where(live, st[0:32], -3.0e38)
    diagonal = iota((8, 8), 0) == iota((8, 8), 1)
    pos = jnp.concatenate(
        [jnp.sum(jnp.where(diagonal, pos_all[g].astype(F32), 0.0), axis=1, keepdims=True) for g in range(4)], axis=0
    ).astype(jnp.int32)
    onehot = jnp.where(lane == pos, 1.0, 0.0)
    top = jnp.max(score, axis=1, keepdims=True)
    expo = jnp.where(live, jnp.exp(score - top), 0.0)
    norm = jnp.sum(expo, axis=1, keepdims=True)
    per_query = top + jnp.log(norm) - jnp.sum(jnp.where(live, score, 0.0) * onehot, axis=1, keepdims=True)
    loss = jnp.sum(per_query, axis=0, keepdims=True) * (1.0 / 32.0) + st[32:33] * reg_weight
    loss_ref[...] = loss
    d_scores = split3(jnp.where(live, expo / norm - onehot, 0.0) * (1.0 / 32.0))
    for b, h in enumerate((1, 0)):
        lanes = [dot_nt(p, doc_lane(h)).astype(BF16) for p in d_scores]
        for k, p in enumerate((0, 1, 0, 2, 1, 0)):
            ds6[pl.ds(k * 32, 32), pl.ds(b * LANES, LANES)] = lanes[p]

    def g_copy(t, half, buf, k, size=VT):
        return pltpu.make_async_copy(
            buf.at[pl.ds(0, size)], gt_hbm.at[at(t, 0, size), pl.ds(half * HALF, HALF)], g_sem.at[k]
        )

    def grad(t, half, buf, k, size=VT):
        if half == 1:
            hi, mid, lo = split3(query_rep(t, 0, size))
            raw_a[pl.ds(0, size)] = dot_tn(jnp.concatenate([hi, hi, mid, hi, mid, lo], axis=0), ds6[...])
        for r in range(size // SUB):
            rows = pl.ds(r * SUB, SUB)
            here = at(t, r * SUB, SUB)
            d_rep = bm[here]
            if half == 1:
                reg = d_rep * (2.0 * reg_weight / 32.0)
                d_rep = raw_a[rows, pl.ds(0, LANES)] + reg
                bm[here] = raw_a[rows, pl.ds(LANES, LANES)] + reg
            total = None
            for b in range(2):
                y = ybuf[here, pl.ds(half * HALF + b * LANES, LANES)]
                d = jnp.where(y > 0.0, d_rep * (1.0 / (1.0 + y)), 0.0)
                total = d if total is None else total + d
                buf[rows, pl.ds(b * LANES, LANES)] = d.astype(BF16)
            raw_b[rows, pl.ds(0, LANES)] = total
        g_copy(t, half, buf, k, size).start()
        for off in range(0, size, LANES):
            width = min(LANES, size - off)
            row = jnp.sum(jnp.transpose(raw_b[pl.ds(off, LANES), pl.ds(0, LANES)]), axis=0, keepdims=True)[:, :width]
            if half == 1:
                db_ref[:, cols(t, off, width)] = row
            else:
                db_ref[:, cols(t, off, width)] += row

    def mm_t(t, buf, acc, size=VT):
        acc[...] += dot_tn(buf[pl.ds(0, size)], wv[at(t, 0, size)]).reshape(acc.shape)

    def backward(half, acc, tick):
        acc[...] = jnp.zeros_like(acc)
        grad(0, half, g_a, 0)

        def body(i, carry):
            t = 2 * i

            @pl.when(i > 0)
            def _():
                g_copy(t - 1, half, g_b, 1).wait()
            grad(t + 1, half, g_b, 1)
            mm_t(t, g_a, acc)
            g_copy(t, half, g_a, 0).wait()
            grad(t + 2, half, g_a, 0)
            mm_t(t + 1, g_b, acc)
            tick(i)
            return carry

        lax.fori_loop(0, (full - 1) // 2, body, 0)
        g_copy(full - 2, half, g_b, 1).wait()
        mm_t(full - 1, g_a, acc)
        grad(full, half, g_b, 1, tail)
        mm_t(full, g_b, acc, tail)
        g_copy(full - 1, half, g_a, 0).wait()
        g_copy(full, half, g_b, 1, tail).wait()

    backward(1, acc1, lambda i: None)
    swap = remote(acc1.at[:, pl.ds(8, 8)], recv1, acc_send, acc_recv, partner)
    swap.start()
    outs = [
        pltpu.make_async_copy(acc1.at[:, pl.ds(0, 8)], send_hbm, out_sem.at[0]),
        pltpu.make_async_copy(acc2.at[:, pl.ds(0, 8)], mine_hbm, out_sem.at[1]),
        pltpu.make_async_copy(acc2.at[:, pl.ds(8, 8)], part_hbm, out_sem.at[2]),
        pltpu.make_async_copy(db_ref.at[0], db_hbm, out_sem.at[4]),
    ]

    def swap_tick(i):
        @pl.when(i == 4)
        def _():
            swap.wait_recv()
            acc1[:, pl.ds(0, 8)] += recv1[...]
            outs[0].start()

    backward(0, acc2, swap_tick)
    outs[1].start()
    outs[2].start()
    outs[3].start()
    for c in outs:
        c.wait()
    hb_out.wait()
    swap.wait_send()
    near.wait_send()
    for c in pk_copies + far + relay + s_copies:
        c.wait_send()


def weight_kernel(gt_ref, hb_ref, out_ref):
    out_ref[...] = dot(gt_ref[...], hb_ref[...]).astype(BF16)


def finish_kernel(mine_ref, part_ref, far_ref, out_ref):
    total = ((mine_ref[...] + part_ref[...]) + far_ref[...]).astype(BF16)
    r, k = iota((ROWS, ROWS), 0), iota((ROWS, ROWS), 1)
    out_ref[...] = dot(one_hot(k == (r & 15) * 8 + (r >> 4)), total).astype(BF16)


def solution(mesh):
    group_size = mesh.shape['tp']
    row_spec = P(('dp', 'tp'))

    def local_step(doc_hidden, doc_mask, query_ids, positive, tok_weight, w_head, b_head):
        docs, doc_len, hidden = doc_hidden.shape
        vocab = w_head.shape[1]
        reg_weight = REG_COEF / (vocab * group_size * doc_len * doc_len)
        tiles = -(-vocab // VT)
        vmem = pl.BlockSpec(memory_space=pltpu.VMEM)
        hbm = pl.BlockSpec(memory_space=pl.ANY)
        dma = pltpu.SemaphoreType.DMA
        block = jax.ShapeDtypeStruct((16, 8, hidden), F32)
        loss, db, gt, hb, send, mine, part = pl.pallas_call(
            functools.partial(head_kernel, reg_weight),
            out_shape=(
                jax.ShapeDtypeStruct((1, LANES), F32),
                jax.ShapeDtypeStruct((vocab,), F32),
                jax.ShapeDtypeStruct((vocab, 2 * HALF), BF16),
                jax.ShapeDtypeStruct((2, HALF, hidden), BF16),
                block, block, block,
            ),
            in_specs=[vmem, vmem, vmem, vmem, hbm, hbm, hbm],
            out_specs=(vmem, hbm, hbm, hbm, hbm, hbm, hbm),
            scratch_shapes=[
                pltpu.VMEM((vocab, hidden), BF16),
                pltpu.VMEM((vocab, 2 * HALF), F32),
                pltpu.VMEM((2, HALF, hidden), BF16),
                pltpu.VMEM((3, ROWS, hidden), BF16),
                pltpu.VMEM((VT, HALF), F32),
                pltpu.VMEM((VT, HALF), F32),
                pltpu.VMEM((VT, HALF), BF16),
                pltpu.VMEM((VT, HALF), BF16),
                pltpu.VMEM((16, 16, hidden), F32),
                pltpu.VMEM((16, 16, hidden), F32),
                pltpu.VMEM((16, 8, hidden), F32),
                pltpu.VMEM((64 * QUERIES, LANES), F32),
                pltpu.VMEM((vocab, LANES), F32),
                pltpu.VMEM((1, vocab), F32),
                pltpu.VMEM((1, vocab), F32),
                pltpu.VMEM((1, vocab), F32),
                pltpu.VMEM((2, 8, LANES), F32),
                pltpu.VMEM((4, 8, 64), jnp.int32),
                pltpu.VMEM((4, 8, 16), jnp.int32),
                pltpu.VMEM((4, 1, 8), jnp.int32),
                pltpu.VMEM((2, 96, LANES), F32),
                pltpu.VMEM((8, LANES), F32),
                pltpu.VMEM((4, 40, LANES), F32),
                pltpu.VMEM((192, HALF), BF16),
                dma((tiles,)), dma((CHUNKS + 1,)), dma((CHUNKS + 1,)), dma((CHUNKS,)), dma((CHUNKS,)),
                dma((9,)), dma((9,)), dma((3,)), dma((3,)), dma, dma, dma((5,)), dma((2,)),
            ],
            compiler_params=pltpu.CompilerParams(
                collective_id=0, has_side_effects=True, vmem_limit_bytes=67_043_328
            ),
            name='head',
        )(
            doc_hidden.reshape(docs * doc_len, hidden), query_ids, doc_mask, positive.reshape(1, 8),
            tok_weight, b_head, w_head.T,
        )

        cross = [(k, (k + 2) % 4) for k in range(4)]
        swap = [(k, k ^ 1) for k in range(4)]
        rows = (docs * doc_len, hidden)
        far = lax.ppermute(send.reshape(rows), 'tp', cross)
        near = lax.ppermute(part.reshape(rows), 'tp', swap)
        step = 800
        d_weight = pl.pallas_call(
            weight_kernel,
            grid=(vocab // step,),
            out_shape=jax.ShapeDtypeStruct((vocab, hidden), BF16),
            in_specs=[
                pl.BlockSpec((step, 2 * HALF), lambda i: (i, 0)),
                pl.BlockSpec((2 * HALF, hidden), lambda i: (0, 0)),
            ],
            out_specs=pl.BlockSpec((step, hidden), lambda i: (i, 0)),
            cost_estimate=pl.CostEstimate(
                flops=2 * hidden * 2 * HALF * vocab, bytes_accessed=50_000_000, transcendentals=0
            ),
            compiler_params=pltpu.CompilerParams(vmem_limit_bytes=67_043_328),
            name='dweight',
        )(gt, hb.reshape(2 * HALF, hidden))
        d_hidden = pl.pallas_call(
            finish_kernel,
            grid=(4,),
            out_shape=jax.ShapeDtypeStruct(rows, BF16),
            in_specs=[pl.BlockSpec((ROWS, hidden // 4), lambda i: (0, i))] * 3,
            out_specs=pl.BlockSpec((ROWS, hidden // 4), lambda i: (0, i)),
            name='finish',
        )(mine.reshape(rows), near, far)
        return loss[0, :1], d_weight.T, db, d_hidden.reshape(docs, doc_len, hidden)

    return jax.shard_map(
        local_step,
        mesh=mesh,
        in_specs=(row_spec, row_spec, row_spec, row_spec, P('tp'), P(None, 'tp'), P('tp')),
        out_specs=(P('dp'), P('dp', 'tp'), row_spec, row_spec),
        check_vma=False,
    )
```

```python
import functools

import jax
import jax.numpy as jnp
from jax import lax
from jax.experimental import pallas as pl
from jax.experimental.pallas import tpu as pltpu
from jax.sharding import PartitionSpec as P

REG_COEF = 32.0
MESH = pl.DeviceIdType.MESH
F32 = jnp.float32
BF16 = jnp.bfloat16
VT = 512
LANES = 128
HALF = 256
ROWS = 128
SUB = 64
CHUNKS = 4
MM_ROWS = 256
MM_COLS = 512
QUERIES = 32
NT_DIMS = (((1,), (1,)), ((), ()))
TN_DIMS = (((0,), (0,)), ((), ()))


def dot(a, b):
    return jnp.dot(a, b, preferred_element_type=F32)


def dot_nt(a, b):
    return lax.dot_general(a, b, NT_DIMS, preferred_element_type=F32)


def dot_tn(a, b):
    return lax.dot_general(a, b, TN_DIMS, preferred_element_type=F32)


def iota(shape, axis):
    return lax.broadcasted_iota(jnp.int32, shape, axis)


def one_hot(cond):
    return jnp.where(cond, 1.0, 0.0).astype(BF16)


def split3(x):
    hi = x.astype(BF16)
    rest = x - hi.astype(F32)
    mid = rest.astype(BF16)
    low = (rest - mid.astype(F32)).astype(BF16)
    return hi, mid, low


def log1p_pos(y):
    return jnp.where(y < 5e-4, y * (1.0 - 0.5 * y), jnp.log(1.0 + y))


def weave(first, second):
    count = max(len(first), 1)
    done = 0
    for k in range(count):
        if first:
            first[k]()
        upto = -(-len(second) * (k + 1) // count)
        for piece in second[done:upto]:
            piece()
        done = upto


def head_kernel(
    reg_weight,
    hid_ref, ids_ref, mask_ref, pos_ref, qw_hbm, bias_hbm, w_hbm,
    loss_ref, db_ref, gt_hbm, hb_hbm, send_hbm, mine_hbm, part_hbm,
    wv, ybuf, hb, land, raw_a, raw_b, g_a, g_b, acc1, acc2, recv1,
    counts, bm, qw_ref, bias_ref, mask_row, ids_all, mask_all, pos_all, s_acc, reg_acc, inbox, ds6,
    w_sem, hid_send, hid_recv, fwd_send, fwd_recv, pk_send, pk_recv, s_send, s_recv, acc_send, acc_recv, out_sem, g_sem,
):
    vocab = wv.shape[0]
    hidden = wv.shape[1]
    full = vocab // VT
    tail = vocab - full * VT
    me = lax.axis_index("tp")
    partner = me + 1 - 2 * lax.rem(me, 2)
    other = lax.rem(me + 2, 4)
    diag = lax.rem(partner + 2, 4)
    slots = (me, partner, other, diag)

    def remote(src, dst, ssem, rsem, dev):
        return pltpu.make_async_remote_copy(src, dst, ssem, rsem, device_id={"tp": dev}, device_id_type=MESH)

    def at(t, off=0, size=VT):
        if isinstance(t, int):
            return pl.ds(t * VT + off, size)
        return pl.ds(pl.multiple_of(t * VT + off, SUB), size)

    def cols(t, off=0, size=VT):
        if isinstance(t, int):
            return pl.ds(t * VT + off, size)
        return pl.ds(pl.multiple_of(t * VT + off, LANES), size)

    def w_copy(t, size=VT):
        return pltpu.make_async_copy(w_hbm.at[at(t, 0, size)], wv.at[at(t, 0, size)], w_sem.at[t])

    rows_in = [
        pltpu.make_async_copy(qw_hbm, qw_ref.at[0], out_sem.at[0]),
        pltpu.make_async_copy(bias_hbm, bias_ref.at[0], out_sem.at[1]),
    ]
    for c in rows_in:
        c.start()
    ahead = 4
    for t in range(ahead):
        w_copy(t).start()

    barrier = pltpu.get_barrier_semaphore()
    for peer in slots[1:]:
        pl.semaphore_signal(barrier, inc=1, device_id={"tp": peer}, device_id_type=MESH)
    pl.semaphore_wait(barrier, 3)

    pk_copies = []
    for k in range(3):
        for i, (src, dst) in enumerate(((ids_ref, ids_all), (mask_ref, mask_all), (pos_ref, pos_all))):
            pk_copies.append(remote(src, dst.at[me], pk_send.at[3 * k + i], pk_recv.at[3 * k + i], slots[k + 1]))
    for c in pk_copies:
        c.start()
    near = remote(hid_ref, land.at[0], hid_send.at[CHUNKS], hid_recv.at[CHUNKS], partner)
    near.start()
    step = ROWS // CHUNKS
    far, relay = [], []
    for k in range(CHUNKS):
        part = pl.ds(k * step, step)
        far.append(remote(hid_ref.at[part], land.at[1, part], hid_send.at[k], hid_recv.at[k], other))
        relay.append(remote(land.at[1, part], land.at[2, part], fwd_send.at[k], fwd_recv.at[k], partner))
    for c in far:
        c.start()

    ones = jnp.ones((16, LANES), BF16)
    sub16 = iota((16, VT), 0)

    def bias_columns(t, size):
        parts = [p.astype(F32) for p in split3(bias_ref[:, cols(t, 0, size)])]
        stack = jnp.zeros((16, size), F32)
        for k in range(3):
            stack = jnp.where(sub16[:, :size] == k, parts[k], stack)
        bm[at(t, 0, size)] = dot_tn(stack.astype(BF16), ones)

    def bias_body(t, carry):
        bias_columns(t, VT)
        return carry

    ids_all[me] = ids_ref[...]
    mask_all[me] = mask_ref[...]
    pos_all[me] = pos_ref[...]
    for c in pk_copies:
        c.wait_recv()

    lane8 = iota((8, LANES), 1)
    for h in range(2):
        total = None
        for k in range(2):
            mask = mask_all[slots[2 * h + k]].astype(F32).astype(BF16)
            spread = dot(mask, one_hot((iota((16, LANES), 1) >> 4) + 8 == iota((16, LANES), 0)))
            piece = jnp.sum(jnp.where((lane8 & 15) == iota((8, LANES), 0) + 8 * k, spread, 0.0), axis=0, keepdims=True)
            total = piece if total is None else total + piece
        mask_row[h] = jnp.broadcast_to(total, (8, LANES))

    ids = jnp.concatenate([ids_all[g] for g in range(4)], axis=0)
    raw_a[pl.ds(0, LANES), pl.ds(0, LANES)] = jnp.zeros((LANES, LANES), F32)
    raw_a[pl.ds(0, QUERIES), pl.ds(0, 64)] = ids.astype(F32)
    ids_t = jnp.transpose(raw_a[pl.ds(0, LANES), pl.ds(0, LANES)])
    high = (ids - me * vocab) >> 7
    low = (ids_t.astype(jnp.int32) - me * vocab) & 127
    for q in range(QUERIES):
        hot_hi = one_hot(iota((64, 64), 0) == high[q:q + 1])
        hot_lo = one_hot(iota((64, LANES), 1) == low[:64, q:q + 1])
        counts[pl.ds(q, 64, QUERIES), :] = dot(hot_hi, hot_lo)
    s_acc[...] = jnp.zeros_like(s_acc)
    reg_acc[...] = jnp.zeros_like(reg_acc)

    def place(half, sources):
        r, k = iota((HALF, ROWS), 0), iota((HALF, ROWS), 1)
        pick = [one_hot((k == (r & 7) * 16 + (r >> 4)) & (((r >> 3) & 1) == s)) for s in range(2)]
        for c in range(hidden // VT):
            block = pl.ds(c * VT, VT)
            mixed = dot(pick[0], sources[0][:, block]) + dot(pick[1], sources[1][:, block])
            hb[half, :, block] = mixed.astype(BF16)

    for c in rows_in:
        c.wait()
    lax.fori_loop(0, full, bias_body, 0)
    bias_columns(full, tail)
    near.wait_recv()
    place(0, (hid_ref, land.at[0]))

    def query_rep(t, off, size):
        out = []
        for c in range(-(-size // LANES)):
            width = min(LANES, size - c * LANES)
            block = t * (VT // LANES) + off // LANES + c
            start = block * QUERIES
            if not isinstance(t, int):
                start = pl.multiple_of(start, QUERIES)
            cnt = counts[pl.ds(start, QUERIES)]
            out.append(cnt[:, :width] * qw_ref[:, cols(t, off + c * LANES, width)])
        return jnp.concatenate(out, axis=1) if len(out) > 1 else out[0]

    def mm(t, half, buf, size=VT):
        def piece(off, depth):
            def run():
                buf[pl.ds(off, depth)] = dot_nt(wv[at(t, off, depth)], hb[half])
            return run
        return [piece(off, min(MM_ROWS, size - off)) for off in range(0, size, MM_ROWS)]

    lane_sub = iota((SUB, LANES), 1)

    def ep(t, half, buf, size=VT):
        def rows_piece(r):
            def run():
                mask = mask_row[half, 0:1]
                rows = pl.ds(r * SUB, SUB)
                here = at(t, r * SUB, SUB)
                col = bm[here]
                bias = col if half == 0 else jnp.broadcast_to(col[:, 0:1], (SUB, LANES))
                acc = None
                for b in range(2):
                    y = jnp.maximum(buf[rows, pl.ds(b * LANES, LANES)] + bias, 0.0)
                    if b == 1:
                        y = y * mask
                    ybuf[here, pl.ds(half * HALF + b * LANES, LANES)] = y
                    act = log1p_pos(y)
                    acc = act if acc is None else acc + act
                buf[rows, pl.ds(0, LANES)] = acc
                total = jnp.sum(acc, axis=1, keepdims=True)
                if half == 0:
                    bm[here] = jnp.where(lane_sub < 64, col, total)
                else:
                    mean = jnp.broadcast_to((total + col[:, 64:65]) * (1.0 / 32.0), (SUB, LANES))
                    bm[here] = mean
                    square = mean * mean
                    reg_acc[...] += jnp.sum(square.reshape(SUB // 8, 8, LANES), axis=0)
            return run

        def score_piece(off):
            def run():
                depth = min(HALF, size - off)
                rq = split3(query_rep(t, off, depth))
                act = split3(buf[pl.ds(off, depth), pl.ds(0, LANES)])
                s_acc[half] += dot(jnp.concatenate(rq, axis=0), act[0])
                s_acc[half, pl.ds(0, 64)] += dot(jnp.concatenate(rq[:2], axis=0), act[1])
                s_acc[half, pl.ds(0, 32)] += dot(rq[0], act[2])
            return run

        out = []
        for off in range(0, size, HALF):
            for r in range(off // SUB, min(off + HALF, size) // SUB):
                out.append(rows_piece(r))
            out.append(score_piece(off))
        return out

    def forward(half, tick):
        first = half == 0
        if first:
            w_copy(0).wait()
        weave(mm(0, half, raw_a), [])

        def body(i, carry):
            t = 2 * i
            if first:
                for u in range(2):
                    @pl.when(t + u + ahead < full)
                    def _():
                        w_copy(t + u + ahead).start()
                @pl.when(i == (full - ahead) // 2)
                def _():
                    w_copy(full, tail).start()
                w_copy(t + 1).wait()
            weave(mm(t + 1, half, raw_b), ep(t, half, raw_a))
            if first:
                w_copy(t + 2).wait()
            weave(mm(t + 2, half, raw_a), ep(t + 1, half, raw_b))
            tick(i)
            return carry

        lax.fori_loop(0, (full - 1) // 2, body, 0)
        if first:
            w_copy(full, tail).wait()
        weave(mm(full, half, raw_b, tail), ep(full - 1, half, raw_a))
        weave([], ep(full, half, raw_b, tail))

    def relay_tick(i):
        for k, when in enumerate((0, 2, 4)):
            @pl.when(i == when)
            def _():
                far[k].wait_recv()
                relay[k].start()

    forward(0, relay_tick)
    far[CHUNKS - 1].wait_recv()
    relay[CHUNKS - 1].start()
    for c in relay:
        c.wait_recv()
    place(1, (land.at[1], land.at[2]))
    hb_out = pltpu.make_async_copy(hb, hb_hbm, out_sem.at[3])
    hb_out.start()
    forward(1, lambda i: None)

    def doc_lane(half):
        k = iota((LANES, LANES), 0)
        owner = jnp.where(((k >> 3) & 1) == 0, slots[2 * half], slots[2 * half + 1])
        return one_hot(iota((LANES, LANES), 1) == owner * 8 + (k & 7))

    scores = None
    for h in range(2):
        mine = s_acc[h, pl.ds(0, 32)] + s_acc[h, pl.ds(32, 32)] + s_acc[h, pl.ds(64, 32)]
        moved = dot(jnp.concatenate(split3(mine), axis=0), doc_lane(h))
        moved = moved[0:32] + moved[32:64] + moved[64:96]
        scores = moved if scores is None else scores + moved
    inbox[me, pl.ds(0, 32)] = scores
    inbox[me, pl.ds(32, 8)] = jnp.broadcast_to(jnp.sum(reg_acc[...], axis=0, keepdims=True), (8, LANES))
    s_copies = [remote(inbox.at[me], inbox.at[me], s_send.at[k], s_recv.at[k], slots[k + 1]) for k in range(3)]
    for c in s_copies:
        c.start()
    for c in s_copies:
        c.wait_recv()
    st = inbox[0] + inbox[1] + inbox[2] + inbox[3]
    lane = iota((32, LANES), 1)
    live = lane < 32
    score = jnp.where(live, st[0:32], -3.0e38)
    diagonal = iota((8, 8), 0) == iota((8, 8), 1)
    pos = jnp.concatenate(
        [jnp.sum(jnp.where(diagonal, pos_all[g].astype(F32), 0.0), axis=1, keepdims=True) for g in range(4)], axis=0
    ).astype(jnp.int32)
    onehot = jnp.where(lane == pos, 1.0, 0.0)
    top = jnp.max(score, axis=1, keepdims=True)
    expo = jnp.where(live, jnp.exp(score - top), 0.0)
    norm = jnp.sum(expo, axis=1, keepdims=True)
    per_query = top + jnp.log(norm) - jnp.sum(jnp.where(live, score, 0.0) * onehot, axis=1, keepdims=True)
    loss = jnp.sum(per_query, axis=0, keepdims=True) * (1.0 / 32.0) + st[32:33] * reg_weight
    loss_ref[...] = loss
    d_scores = split3(jnp.where(live, expo / norm - onehot, 0.0) * (1.0 / 32.0))
    for b, h in enumerate((1, 0)):
        lanes = [dot_nt(p, doc_lane(h)).astype(BF16) for p in d_scores]
        for k, p in enumerate((0, 1, 0, 2, 1, 0)):
            ds6[pl.ds(k * 32, 32), pl.ds(b * LANES, LANES)] = lanes[p]

    def g_copy(t, half, buf, k, size=VT):
        return pltpu.make_async_copy(
            buf.at[pl.ds(0, size)], gt_hbm.at[at(t, 0, size), pl.ds(half * HALF, HALF)], g_sem.at[k]
        )

    def grad(t, half, buf, k, size=VT):
        def setup(off):
            def run():
                depth = min(HALF, size - off)
                hi, mid, lo = split3(query_rep(t, off, depth))
                raw_a[pl.ds(off, depth)] = dot_tn(jnp.concatenate([hi, hi, mid, hi, mid, lo], axis=0), ds6[...])
            return run

        def rows_piece(r):
            def run():
                rows = pl.ds(r * SUB, SUB)
                here = at(t, r * SUB, SUB)
                d_rep = bm[here]
                if half == 1:
                    reg = d_rep * (2.0 * reg_weight / 32.0)
                    d_rep = raw_a[rows, pl.ds(0, LANES)] + reg
                    bm[here] = raw_a[rows, pl.ds(LANES, LANES)] + reg
                total = None
                for b in range(2):
                    y = ybuf[here, pl.ds(half * HALF + b * LANES, LANES)]
                    d = jnp.where(y > 0.0, d_rep * (1.0 / (1.0 + y)), 0.0)
                    total = d if total is None else total + d
                    buf[rows, pl.ds(b * LANES, LANES)] = d.astype(BF16)
                raw_b[rows, pl.ds(0, LANES)] = total
            return run

        def finish():
            g_copy(t, half, buf, k, size).start()
            for off in range(0, size, LANES):
                width = min(LANES, size - off)
                row = jnp.sum(jnp.transpose(raw_b[pl.ds(off, LANES), pl.ds(0, LANES)]), axis=0, keepdims=True)[:, :width]
                if half == 1:
                    db_ref[:, cols(t, off, width)] = row
                else:
                    db_ref[:, cols(t, off, width)] += row

        out = []
        for off in range(0, size, HALF):
            if half == 1:
                out.append(setup(off))
            out += [rows_piece(r) for r in range(off // SUB, min(off + HALF, size) // SUB)]
        return out + [finish]

    def mm_t(t, buf, acc, size=VT):
        def piece(n):
            def run():
                block = pl.ds(n * MM_COLS, MM_COLS)
                acc[:, :, block] += dot_tn(buf[pl.ds(0, size)], wv[at(t, 0, size), block]).reshape(16, 16, MM_COLS)
            return run
        return [piece(n) for n in range(hidden // MM_COLS)]

    def backward(half, acc, tick):
        acc[...] = jnp.zeros_like(acc)
        weave([], grad(0, half, g_a, 0))

        def body(i, carry):
            t = 2 * i

            @pl.when(i > 0)
            def _():
                g_copy(t - 1, half, g_b, 1).wait()
            weave(mm_t(t, g_a, acc), grad(t + 1, half, g_b, 1))
            g_copy(t, half, g_a, 0).wait()
            weave(mm_t(t + 1, g_b, acc), grad(t + 2, half, g_a, 0))
            tick(i)
            return carry

        lax.fori_loop(0, (full - 1) // 2, body, 0)
        g_copy(full - 2, half, g_b, 1).wait()
        weave(mm_t(full - 1, g_a, acc), grad(full, half, g_b, 1, tail))
        weave(mm_t(full, g_b, acc, tail), [])
        g_copy(full - 1, half, g_a, 0).wait()
        g_copy(full, half, g_b, 1, tail).wait()

    backward(1, acc1, lambda i: None)
    swap = remote(acc1.at[:, pl.ds(8, 8)], recv1, acc_send, acc_recv, partner)
    swap.start()
    outs = [
        pltpu.make_async_copy(acc1.at[:, pl.ds(0, 8)], send_hbm, out_sem.at[0]),
        pltpu.make_async_copy(acc2.at[:, pl.ds(0, 8)], mine_hbm, out_sem.at[1]),
        pltpu.make_async_copy(acc2.at[:, pl.ds(8, 8)], part_hbm, out_sem.at[2]),
    ]

    def swap_tick(i):
        @pl.when(i == 4)
        def _():
            swap.wait_recv()
            acc1[:, pl.ds(0, 8)] += recv1[...]
            outs[0].start()

    backward(0, acc2, swap_tick)
    outs[1].start()
    outs[2].start()
    for c in outs:
        c.wait()
    hb_out.wait()
    swap.wait_send()
    near.wait_send()
    for c in pk_copies + far + relay + s_copies:
        c.wait_send()


def weight_kernel(gt_ref, hb_ref, db_ref, out_ref, db_hbm, sem):
    copy = pltpu.make_async_copy(db_ref.at[0], db_hbm, sem)
    pl.when(pl.program_id(0) == 0)(copy.start)
    pl.when(pl.program_id(0) == pl.num_programs(0) - 1)(copy.wait)
    out_ref[...] = dot(gt_ref[...], hb_ref[...]).astype(BF16)


def finish_kernel(mine_ref, part_ref, far_ref, out_ref):
    total = ((mine_ref[...] + part_ref[...]) + far_ref[...]).astype(BF16)
    r, k = iota((ROWS, ROWS), 0), iota((ROWS, ROWS), 1)
    out_ref[...] = dot(one_hot(k == (r & 15) * 8 + (r >> 4)), total).astype(BF16)


def solution(mesh):
    group_size = mesh.shape['tp']
    row_spec = P(('dp', 'tp'))

    def local_step(doc_hidden, doc_mask, query_ids, positive, tok_weight, w_head, b_head):
        docs, doc_len, hidden = doc_hidden.shape
        vocab = w_head.shape[1]
        reg_weight = REG_COEF / (vocab * group_size * doc_len * doc_len)
        tiles = -(-vocab // VT)
        vmem = pl.BlockSpec(memory_space=pltpu.VMEM)
        hbm = pl.BlockSpec(memory_space=pl.ANY)
        dma = pltpu.SemaphoreType.DMA
        block = jax.ShapeDtypeStruct((16, 8, hidden), F32)
        loss, db, gt, hb, send, mine, part = pl.pallas_call(
            functools.partial(head_kernel, reg_weight),
            out_shape=(
                jax.ShapeDtypeStruct((1, LANES), F32),
                jax.ShapeDtypeStruct((1, vocab), F32),
                jax.ShapeDtypeStruct((vocab, 2 * HALF), BF16),
                jax.ShapeDtypeStruct((2, HALF, hidden), BF16),
                block, block, block,
            ),
            in_specs=[vmem, vmem, vmem, vmem, hbm, hbm, hbm],
            out_specs=(vmem, vmem, hbm, hbm, hbm, hbm, hbm),
            scratch_shapes=[
                pltpu.VMEM((vocab, hidden), BF16),
                pltpu.VMEM((vocab, 2 * HALF), F32),
                pltpu.VMEM((2, HALF, hidden), BF16),
                pltpu.VMEM((3, ROWS, hidden), BF16),
                pltpu.VMEM((VT, HALF), F32),
                pltpu.VMEM((VT, HALF), F32),
                pltpu.VMEM((VT, HALF), BF16),
                pltpu.VMEM((VT, HALF), BF16),
                pltpu.VMEM((16, 16, hidden), F32),
                pltpu.VMEM((16, 16, hidden), F32),
                pltpu.VMEM((16, 8, hidden), F32),
                pltpu.VMEM((64 * QUERIES, LANES), F32),
                pltpu.VMEM((vocab, LANES), F32),
                pltpu.VMEM((1, vocab), F32),
                pltpu.VMEM((1, vocab), F32),
                pltpu.VMEM((2, 8, LANES), F32),
                pltpu.VMEM((4, 8, 64), jnp.int32),
                pltpu.VMEM((4, 8, 16), jnp.int32),
                pltpu.VMEM((4, 1, 8), jnp.int32),
                pltpu.VMEM((2, 96, LANES), F32),
                pltpu.VMEM((8, LANES), F32),
                pltpu.VMEM((4, 40, LANES), F32),
                pltpu.VMEM((192, HALF), BF16),
                dma((tiles,)), dma((CHUNKS + 1,)), dma((CHUNKS + 1,)), dma((CHUNKS,)), dma((CHUNKS,)),
                dma((9,)), dma((9,)), dma((3,)), dma((3,)), dma, dma, dma((5,)), dma((2,)),
            ],
            compiler_params=pltpu.CompilerParams(
                collective_id=0, has_side_effects=True, vmem_limit_bytes=67_043_328
            ),
            name='head',
        )(
            doc_hidden.reshape(docs * doc_len, hidden), query_ids, doc_mask, positive.reshape(1, 8),
            tok_weight, b_head, w_head.T,
        )

        cross = [(k, (k + 2) % 4) for k in range(4)]
        swap = [(k, k ^ 1) for k in range(4)]
        rows = (docs * doc_len, hidden)
        far = lax.ppermute(send.reshape(rows), 'tp', cross)
        near = lax.ppermute(part.reshape(rows), 'tp', swap)
        step = 800
        d_weight, d_bias = pl.pallas_call(
            weight_kernel,
            grid=(vocab // step,),
            out_shape=(jax.ShapeDtypeStruct((vocab, hidden), BF16), jax.ShapeDtypeStruct((vocab,), F32)),
            in_specs=[
                pl.BlockSpec((step, 2 * HALF), lambda i: (i, 0)),
                pl.BlockSpec((2 * HALF, hidden), lambda i: (0, 0), pipeline_mode=pl.Buffered(1)),
                vmem,
            ],
            out_specs=(pl.BlockSpec((step, hidden), lambda i: (i, 0)), hbm),
            scratch_shapes=[dma],
            cost_estimate=pl.CostEstimate(
                flops=2 * hidden * 2 * HALF * vocab, bytes_accessed=50_000_000, transcendentals=0
            ),
            compiler_params=pltpu.CompilerParams(vmem_limit_bytes=67_043_328),
            name='dweight',
        )(gt, hb.reshape(2 * HALF, hidden), db)
        d_hidden = pl.pallas_call(
            finish_kernel,
            out_shape=jax.ShapeDtypeStruct(rows, BF16),
            name='finish',
        )(mine.reshape(rows), near, far)
        return loss[0, :1], d_weight.T, d_bias, d_hidden.reshape(docs, doc_len, hidden)

    return jax.shard_map(
        local_step,
        mesh=mesh,
        in_specs=(row_spec, row_spec, row_spec, row_spec, P('tp'), P(None, 'tp'), P('tp')),
        out_specs=(P('dp'), P('dp', 'tp'), row_spec, row_spec),
        check_vma=False,
    )
```

```python
import functools

import jax
import jax.numpy as jnp
from jax import lax
from jax.experimental import pallas as pl
from jax.experimental.pallas import tpu as pltpu
from jax.sharding import PartitionSpec as P

REG_COEF = 32.0
MESH = pl.DeviceIdType.MESH
F32 = jnp.float32
BF16 = jnp.bfloat16
VT = 512
LANES = 128
HALF = 256
ROWS = 128
SUB = 64
CHUNKS = 4
EARLY = 256
MM_ROWS = 256
MM_COLS = 512
QUERIES = 32
NT_DIMS = (((1,), (1,)), ((), ()))
TN_DIMS = (((0,), (0,)), ((), ()))


def dot(a, b):
    return jnp.dot(a, b, preferred_element_type=F32)


def dot_nt(a, b):
    return lax.dot_general(a, b, NT_DIMS, preferred_element_type=F32)


def dot_tn(a, b):
    return lax.dot_general(a, b, TN_DIMS, preferred_element_type=F32)


def iota(shape, axis):
    return lax.broadcasted_iota(jnp.int32, shape, axis)


def one_hot(cond):
    return jnp.where(cond, 1.0, 0.0).astype(BF16)


def split3(x):
    hi = x.astype(BF16)
    rest = x - hi.astype(F32)
    mid = rest.astype(BF16)
    low = (rest - mid.astype(F32)).astype(BF16)
    return hi, mid, low


def log1p_pos(y):
    return jnp.where(y < 5e-4, y * (1.0 - 0.5 * y), jnp.log(1.0 + y))


def weave(first, second):
    count = max(len(first), 1)
    done = 0
    for k in range(count):
        if first:
            first[k]()
        upto = -(-len(second) * (k + 1) // count)
        for piece in second[done:upto]:
            piece()
        done = upto


def head_kernel(
    reg_weight,
    hid_ref, ids_ref, mask_ref, pos_ref, qw_hbm, bias_hbm, w_hbm,
    loss_ref, db_ref, gt_hbm, hb_hbm, send_hbm, mine_hbm, part_hbm,
    wv, ybuf, hb, land, raw_a, raw_b, g_a, g_b, acc1, acc2, recv1,
    counts, bm, qw_ref, bias_ref, mask_row, ids_all, mask_all, pos_all, s_acc, reg_acc, inbox, ds6,
    w_sem, hid_send, hid_recv, fwd_send, fwd_recv, pk_send, pk_recv, s_send, s_recv, acc_send, acc_recv, far_send, far_recv, free_sem, out_sem, g_sem,
):
    vocab = wv.shape[0]
    hidden = wv.shape[1]
    full = vocab // VT
    tail = vocab - full * VT
    me = lax.axis_index("tp")
    partner = me + 1 - 2 * lax.rem(me, 2)
    other = lax.rem(me + 2, 4)
    diag = lax.rem(partner + 2, 4)
    slots = (me, partner, other, diag)

    def remote(src, dst, ssem, rsem, dev):
        return pltpu.make_async_remote_copy(src, dst, ssem, rsem, device_id={"tp": dev}, device_id_type=MESH)

    def at(t, off=0, size=VT):
        if isinstance(t, int):
            return pl.ds(t * VT + off, size)
        return pl.ds(pl.multiple_of(t * VT + off, SUB), size)

    def cols(t, off=0, size=VT):
        if isinstance(t, int):
            return pl.ds(t * VT + off, size)
        return pl.ds(pl.multiple_of(t * VT + off, LANES), size)

    def w_copy(t, size=VT):
        return pltpu.make_async_copy(w_hbm.at[at(t, 0, size)], wv.at[at(t, 0, size)], w_sem.at[t])

    rows_in = [
        pltpu.make_async_copy(qw_hbm, qw_ref.at[0], out_sem.at[0]),
        pltpu.make_async_copy(bias_hbm, bias_ref.at[0], out_sem.at[1]),
    ]
    for c in rows_in:
        c.start()
    ahead = 4
    for t in range(ahead):
        w_copy(t).start()

    barrier = pltpu.get_barrier_semaphore()
    for peer in slots[1:]:
        pl.semaphore_signal(barrier, inc=1, device_id={"tp": peer}, device_id_type=MESH)
    pl.semaphore_wait(barrier, 3)

    pk_copies = []
    for k in range(3):
        for i, (src, dst) in enumerate(((ids_ref, ids_all), (mask_ref, mask_all), (pos_ref, pos_all))):
            pk_copies.append(remote(src, dst.at[me], pk_send.at[3 * k + i], pk_recv.at[3 * k + i], slots[k + 1]))
    for c in pk_copies:
        c.start()
    near = remote(hid_ref, land.at[0], hid_send.at[CHUNKS], hid_recv.at[CHUNKS], partner)
    near.start()
    step = ROWS // CHUNKS
    far, relay = [], []
    for k in range(CHUNKS):
        part = pl.ds(k * step, step)
        far.append(remote(hid_ref.at[part], land.at[1, part], hid_send.at[k], hid_recv.at[k], other))
        relay.append(remote(land.at[1, part], land.at[2, part], fwd_send.at[k], fwd_recv.at[k], partner))
    for c in far:
        c.start()

    ones = jnp.ones((16, LANES), BF16)
    sub16 = iota((16, VT), 0)

    def bias_columns(t, size):
        parts = [p.astype(F32) for p in split3(bias_ref[:, cols(t, 0, size)])]
        stack = jnp.zeros((16, size), F32)
        for k in range(3):
            stack = jnp.where(sub16[:, :size] == k, parts[k], stack)
        bm[at(t, 0, size)] = dot_tn(stack.astype(BF16), ones)

    def bias_piece(t, size=VT):
        return [functools.partial(bias_columns, t, size)]

    ids_all[me] = ids_ref[...]
    mask_all[me] = mask_ref[...]
    pos_all[me] = pos_ref[...]
    for c in pk_copies:
        c.wait_recv()

    lane8 = iota((8, LANES), 1)
    for h in range(2):
        total = None
        for k in range(2):
            mask = mask_all[slots[2 * h + k]].astype(F32).astype(BF16)
            spread = dot(mask, one_hot((iota((16, LANES), 1) >> 4) + 8 == iota((16, LANES), 0)))
            piece = jnp.sum(jnp.where((lane8 & 15) == iota((8, LANES), 0) + 8 * k, spread, 0.0), axis=0, keepdims=True)
            total = piece if total is None else total + piece
        mask_row[h] = jnp.broadcast_to(total, (8, LANES))

    ids = jnp.concatenate([ids_all[g] for g in range(4)], axis=0)
    raw_a[pl.ds(0, LANES), pl.ds(0, LANES)] = jnp.zeros((LANES, LANES), F32)
    raw_a[pl.ds(0, QUERIES), pl.ds(0, 64)] = ids.astype(F32)
    ids_t = jnp.transpose(raw_a[pl.ds(0, LANES), pl.ds(0, LANES)])
    high = (ids - me * vocab) >> 7
    low = (ids_t.astype(jnp.int32) - me * vocab) & 127
    for q in range(QUERIES):
        hot_hi = one_hot(iota((64, 64), 0) == high[q:q + 1])
        hot_lo = one_hot(iota((64, LANES), 1) == low[:64, q:q + 1])
        counts[pl.ds(q, 64, QUERIES), :] = dot(hot_hi, hot_lo)
    s_acc[...] = jnp.zeros_like(s_acc)
    reg_acc[...] = jnp.zeros_like(reg_acc)

    def place(half, sources):
        r, k = iota((HALF, ROWS), 0), iota((HALF, ROWS), 1)
        pick = [one_hot((k == (r & 7) * 16 + (r >> 4)) & (((r >> 3) & 1) == s)) for s in range(2)]
        for c in range(hidden // VT):
            block = pl.ds(c * VT, VT)
            mixed = dot(pick[0], sources[0][:, block]) + dot(pick[1], sources[1][:, block])
            hb[half, :, block] = mixed.astype(BF16)

    for c in rows_in:
        c.wait()
    bias_columns(0, VT)
    near.wait_recv()
    place(0, (hid_ref, land.at[0]))

    def query_rep(t, off, size):
        out = []
        for c in range(-(-size // LANES)):
            width = min(LANES, size - c * LANES)
            block = t * (VT // LANES) + off // LANES + c
            start = block * QUERIES
            if not isinstance(t, int):
                start = pl.multiple_of(start, QUERIES)
            cnt = counts[pl.ds(start, QUERIES)]
            out.append(cnt[:, :width] * qw_ref[:, cols(t, off + c * LANES, width)])
        return jnp.concatenate(out, axis=1) if len(out) > 1 else out[0]

    def mm(t, half, buf, size=VT):
        def piece(off, depth):
            def run():
                buf[pl.ds(off, depth)] = dot_nt(wv[at(t, off, depth)], hb[half])
            return run
        return [piece(off, min(MM_ROWS, size - off)) for off in range(0, size, MM_ROWS)]

    lane_sub = iota((SUB, LANES), 1)

    def ep(t, half, buf, size=VT):
        def rows_piece(r):
            def run():
                mask = mask_row[half, 0:1]
                rows = pl.ds(r * SUB, SUB)
                here = at(t, r * SUB, SUB)
                col = bm[here]
                bias = col if half == 0 else jnp.broadcast_to(col[:, 0:1], (SUB, LANES))
                acc = None
                for b in range(2):
                    y = jnp.maximum(buf[rows, pl.ds(b * LANES, LANES)] + bias, 0.0)
                    if b == 1:
                        y = y * mask
                    ybuf[here, pl.ds(half * HALF + b * LANES, LANES)] = y
                    act = log1p_pos(y)
                    acc = act if acc is None else acc + act
                buf[rows, pl.ds(0, LANES)] = acc
                total = jnp.sum(acc, axis=1, keepdims=True)
                if half == 0:
                    bm[here] = jnp.where(lane_sub < 64, col, total)
                else:
                    mean = jnp.broadcast_to((total + col[:, 64:65]) * (1.0 / 32.0), (SUB, LANES))
                    bm[here] = mean
                    square = mean * mean
                    reg_acc[...] += jnp.sum(square.reshape(SUB // 8, 8, LANES), axis=0)
            return run

        def score_piece(off):
            def run():
                depth = min(HALF, size - off)
                rq = split3(query_rep(t, off, depth))
                act = split3(buf[pl.ds(off, depth), pl.ds(0, LANES)])
                s_acc[half] += dot(jnp.concatenate(rq, axis=0), act[0])
                s_acc[half, pl.ds(0, 64)] += dot(jnp.concatenate(rq[:2], axis=0), act[1])
                s_acc[half, pl.ds(0, 32)] += dot(rq[0], act[2])
            return run

        out = []
        for off in range(0, size, HALF):
            for r in range(off // SUB, min(off + HALF, size) // SUB):
                out.append(rows_piece(r))
            out.append(score_piece(off))
        return out

    def forward(half, tick):
        first = half == 0
        if first:
            w_copy(0).wait()
        weave(mm(0, half, raw_a), [])

        def body(i, carry):
            t = 2 * i
            if first:
                for u in range(2):
                    @pl.when(t + u + ahead < full)
                    def _():
                        w_copy(t + u + ahead).start()
                @pl.when(i == (full - ahead) // 2)
                def _():
                    w_copy(full, tail).start()
                w_copy(t + 1).wait()
            weave(mm(t + 1, half, raw_b), (bias_piece(t + 1) if first else []) + ep(t, half, raw_a))
            if first:
                w_copy(t + 2).wait()
            weave(mm(t + 2, half, raw_a), (bias_piece(t + 2) if first else []) + ep(t + 1, half, raw_b))
            tick(i)
            return carry

        lax.fori_loop(0, (full - 1) // 2, body, 0)
        if first:
            w_copy(full, tail).wait()
        weave(mm(full, half, raw_b, tail), (bias_piece(full, tail) if first else []) + ep(full - 1, half, raw_a))
        weave([], ep(full, half, raw_b, tail))

    def relay_tick(i):
        for k, when in enumerate((0, 2, 4)):
            @pl.when(i == when)
            def _():
                far[k].wait_recv()
                relay[k].start()

    forward(0, relay_tick)
    far[CHUNKS - 1].wait_recv()
    relay[CHUNKS - 1].start()
    for c in relay:
        c.wait_recv()
    place(1, (land.at[1], land.at[2]))
    hb_out = pltpu.make_async_copy(hb, hb_hbm, out_sem.at[3])
    hb_out.start()
    forward(1, lambda i: None)

    def doc_lane(half):
        k = iota((LANES, LANES), 0)
        owner = jnp.where(((k >> 3) & 1) == 0, slots[2 * half], slots[2 * half + 1])
        return one_hot(iota((LANES, LANES), 1) == owner * 8 + (k & 7))

    scores = None
    for h in range(2):
        mine = s_acc[h, pl.ds(0, 32)] + s_acc[h, pl.ds(32, 32)] + s_acc[h, pl.ds(64, 32)]
        moved = dot(jnp.concatenate(split3(mine), axis=0), doc_lane(h))
        moved = moved[0:32] + moved[32:64] + moved[64:96]
        scores = moved if scores is None else scores + moved
    inbox[me, pl.ds(0, 32)] = scores
    inbox[me, pl.ds(32, 8)] = jnp.broadcast_to(jnp.sum(reg_acc[...], axis=0, keepdims=True), (8, LANES))
    s_copies = [remote(inbox.at[me], inbox.at[me], s_send.at[k], s_recv.at[k], slots[k + 1]) for k in range(3)]
    for c in s_copies:
        c.start()
    for c in s_copies:
        c.wait_recv()
    st = inbox[0] + inbox[1] + inbox[2] + inbox[3]
    lane = iota((32, LANES), 1)
    live = lane < 32
    score = jnp.where(live, st[0:32], -3.0e38)
    diagonal = iota((8, 8), 0) == iota((8, 8), 1)
    pos = jnp.concatenate(
        [jnp.sum(jnp.where(diagonal, pos_all[g].astype(F32), 0.0), axis=1, keepdims=True) for g in range(4)], axis=0
    ).astype(jnp.int32)
    onehot = jnp.where(lane == pos, 1.0, 0.0)
    top = jnp.max(score, axis=1, keepdims=True)
    expo = jnp.where(live, jnp.exp(score - top), 0.0)
    norm = jnp.sum(expo, axis=1, keepdims=True)
    per_query = top + jnp.log(norm) - jnp.sum(jnp.where(live, score, 0.0) * onehot, axis=1, keepdims=True)
    loss = jnp.sum(per_query, axis=0, keepdims=True) * (1.0 / 32.0) + st[32:33] * reg_weight
    loss_ref[...] = loss
    d_scores = split3(jnp.where(live, expo / norm - onehot, 0.0) * (1.0 / 32.0))
    for b, h in enumerate((1, 0)):
        lanes = [dot_nt(p, doc_lane(h)).astype(BF16) for p in d_scores]
        for k, p in enumerate((0, 1, 0, 2, 1, 0)):
            ds6[pl.ds(k * 32, 32), pl.ds(b * LANES, LANES)] = lanes[p]

    def g_copy(t, half, buf, k, size=VT):
        return pltpu.make_async_copy(
            buf.at[pl.ds(0, size)], gt_hbm.at[at(t, 0, size), pl.ds(half * HALF, HALF)], g_sem.at[k]
        )

    def grad(t, half, buf, k, size=VT):
        def setup(off):
            def run():
                depth = min(HALF, size - off)
                hi, mid, lo = split3(query_rep(t, off, depth))
                raw_a[pl.ds(off, depth)] = dot_tn(jnp.concatenate([hi, hi, mid, hi, mid, lo], axis=0), ds6[...])
            return run

        def rows_piece(r):
            def run():
                rows = pl.ds(r * SUB, SUB)
                here = at(t, r * SUB, SUB)
                d_rep = bm[here]
                if half == 1:
                    reg = d_rep * (2.0 * reg_weight / 32.0)
                    d_rep = raw_a[rows, pl.ds(0, LANES)] + reg
                    bm[here] = raw_a[rows, pl.ds(LANES, LANES)] + reg
                total = None
                for b in range(2):
                    y = ybuf[here, pl.ds(half * HALF + b * LANES, LANES)]
                    d = jnp.where(y > 0.0, d_rep * (1.0 / (1.0 + y)), 0.0)
                    total = d if total is None else total + d
                    buf[rows, pl.ds(b * LANES, LANES)] = d.astype(BF16)
                raw_b[rows, pl.ds(0, LANES)] = total
            return run

        def finish():
            g_copy(t, half, buf, k, size).start()
            for off in range(0, size, LANES):
                width = min(LANES, size - off)
                row = jnp.sum(jnp.transpose(raw_b[pl.ds(off, LANES), pl.ds(0, LANES)]), axis=0, keepdims=True)[:, :width]
                if half == 1:
                    db_ref[:, cols(t, off, width)] = row
                else:
                    db_ref[:, cols(t, off, width)] += row

        out = []
        for off in range(0, size, HALF):
            if half == 1:
                out.append(setup(off))
            out += [rows_piece(r) for r in range(off // SUB, min(off + HALF, size) // SUB)]
        return out + [finish]

    def mm_t(t, buf, acc, size=VT):
        def piece(n):
            def run():
                block = pl.ds(n * MM_COLS, MM_COLS)
                acc[:, :, block] += dot_tn(buf[pl.ds(0, size)], wv[at(t, 0, size), block]).reshape(16, 16, MM_COLS)
            return run
        return [piece(n) for n in range(hidden // MM_COLS)]

    def backward(half, acc, tick):
        acc[...] = jnp.zeros_like(acc)
        weave([], grad(0, half, g_a, 0))

        def body(i, carry):
            t = 2 * i

            @pl.when(i > 0)
            def _():
                g_copy(t - 1, half, g_b, 1).wait()
            weave(mm_t(t, g_a, acc), grad(t + 1, half, g_b, 1))
            g_copy(t, half, g_a, 0).wait()
            weave(mm_t(t + 1, g_b, acc), grad(t + 2, half, g_a, 0))
            tick(i)
            return carry

        lax.fori_loop(0, (full - 1) // 2, body, 0)
        g_copy(full - 2, half, g_b, 1).wait()
        weave(mm_t(full - 1, g_a, acc), grad(full, half, g_b, 1, tail))
        weave(mm_t(full, g_b, acc, tail), [])
        g_copy(full - 1, half, g_a, 0).wait()
        g_copy(full, half, g_b, 1, tail).wait()

    backward(1, acc1, lambda i: None)
    swap = remote(acc1.at[:, pl.ds(8, 8)], recv1, acc_send, acc_recv, partner)
    swap.start()
    outs = [
        pltpu.make_async_copy(acc1.at[:, pl.ds(0, 8), pl.ds(EARLY, hidden - EARLY)], send_hbm, out_sem.at[0]),
        pltpu.make_async_copy(acc2.at[:, pl.ds(0, 8)], mine_hbm, out_sem.at[1]),
        pltpu.make_async_copy(acc2.at[:, pl.ds(8, 8)], part_hbm, out_sem.at[2]),
    ]

    early = remote(acc1.at[:, pl.ds(0, 8), pl.ds(0, EARLY)], recv1.at[:, :, pl.ds(0, EARLY)], far_send, far_recv, other)

    def swap_tick(i):
        @pl.when(i == 1)
        def _():
            swap.wait_recv()
            acc1[:, pl.ds(0, 8)] += recv1[...]
            outs[0].start()
            pl.semaphore_signal(free_sem, inc=1, device_id={"tp": other}, device_id_type=MESH)

        @pl.when(i == 2)
        def _():
            pl.semaphore_wait(free_sem, 1)
            early.start()

    backward(0, acc2, swap_tick)
    outs[2].start()
    early.wait_recv()
    acc2[:, pl.ds(0, 8), pl.ds(0, EARLY)] += recv1[:, :, pl.ds(0, EARLY)]
    outs[1].start()
    for c in outs:
        c.wait()
    hb_out.wait()
    swap.wait_send()
    early.wait_send()
    near.wait_send()
    for c in pk_copies + far + relay + s_copies:
        c.wait_send()


def weight_kernel(gt_ref, hb_ref, db_ref, out_ref, db_hbm, sem):
    copy = pltpu.make_async_copy(db_ref.at[0], db_hbm, sem)
    pl.when(pl.program_id(0) == 0)(copy.start)
    pl.when(pl.program_id(0) == pl.num_programs(0) - 1)(copy.wait)
    out_ref[...] = dot(gt_ref[...], hb_ref[...]).astype(BF16)


def finish_kernel(mine_ref, part_ref, far_ref, out_ref):
    r, k = iota((ROWS, ROWS), 0), iota((ROWS, ROWS), 1)
    perm = one_hot(k == (r & 15) * 8 + (r >> 4))
    total = mine_ref[...] + part_ref[...]
    early, late = pl.ds(0, EARLY), pl.ds(EARLY, total.shape[1] - EARLY)
    out_ref[:, early] = dot(perm, total[:, :EARLY].astype(BF16)).astype(BF16)
    out_ref[:, late] = dot(perm, (total[:, EARLY:] + far_ref[...]).astype(BF16)).astype(BF16)


def solution(mesh):
    group_size = mesh.shape['tp']
    row_spec = P(('dp', 'tp'))

    def local_step(doc_hidden, doc_mask, query_ids, positive, tok_weight, w_head, b_head):
        docs, doc_len, hidden = doc_hidden.shape
        vocab = w_head.shape[1]
        reg_weight = REG_COEF / (vocab * group_size * doc_len * doc_len)
        tiles = -(-vocab // VT)
        vmem = pl.BlockSpec(memory_space=pltpu.VMEM)
        hbm = pl.BlockSpec(memory_space=pl.ANY)
        dma = pltpu.SemaphoreType.DMA
        block = jax.ShapeDtypeStruct((16, 8, hidden), F32)
        loss, db, gt, hb, send, mine, part = pl.pallas_call(
            functools.partial(head_kernel, reg_weight),
            out_shape=(
                jax.ShapeDtypeStruct((1, LANES), F32),
                jax.ShapeDtypeStruct((1, vocab), F32),
                jax.ShapeDtypeStruct((vocab, 2 * HALF), BF16),
                jax.ShapeDtypeStruct((2, HALF, hidden), BF16),
                jax.ShapeDtypeStruct((16, 8, hidden - EARLY), F32), block, block,
            ),
            in_specs=[vmem, vmem, vmem, vmem, hbm, hbm, hbm],
            out_specs=(vmem, vmem, hbm, hbm, hbm, hbm, hbm),
            scratch_shapes=[
                pltpu.VMEM((vocab, hidden), BF16),
                pltpu.VMEM((vocab, 2 * HALF), F32),
                pltpu.VMEM((2, HALF, hidden), BF16),
                pltpu.VMEM((3, ROWS, hidden), BF16),
                pltpu.VMEM((VT, HALF), F32),
                pltpu.VMEM((VT, HALF), F32),
                pltpu.VMEM((VT, HALF), BF16),
                pltpu.VMEM((VT, HALF), BF16),
                pltpu.VMEM((16, 16, hidden), F32),
                pltpu.VMEM((16, 16, hidden), F32),
                pltpu.VMEM((16, 8, hidden), F32),
                pltpu.VMEM((64 * QUERIES, LANES), F32),
                pltpu.VMEM((vocab, LANES), F32),
                pltpu.VMEM((1, vocab), F32),
                pltpu.VMEM((1, vocab), F32),
                pltpu.VMEM((2, 8, LANES), F32),
                pltpu.VMEM((4, 8, 64), jnp.int32),
                pltpu.VMEM((4, 8, 16), jnp.int32),
                pltpu.VMEM((4, 1, 8), jnp.int32),
                pltpu.VMEM((2, 96, LANES), F32),
                pltpu.VMEM((8, LANES), F32),
                pltpu.VMEM((4, 40, LANES), F32),
                pltpu.VMEM((192, HALF), BF16),
                dma((tiles,)), dma((CHUNKS + 1,)), dma((CHUNKS + 1,)), dma((CHUNKS,)), dma((CHUNKS,)),
                dma((9,)), dma((9,)), dma((3,)), dma((3,)), dma, dma, dma, dma, pltpu.SemaphoreType.REGULAR, dma((5,)), dma((2,)),
            ],
            compiler_params=pltpu.CompilerParams(
                collective_id=0, has_side_effects=True, vmem_limit_bytes=67_043_328
            ),
            name='head',
        )(
            doc_hidden.reshape(docs * doc_len, hidden), query_ids, doc_mask, positive.reshape(1, 8),
            tok_weight, b_head, w_head.T,
        )

        cross = [(k, (k + 2) % 4) for k in range(4)]
        swap = [(k, k ^ 1) for k in range(4)]
        rows = (docs * doc_len, hidden)
        far = lax.ppermute(send.reshape(rows[0], hidden - EARLY), 'tp', cross)
        near = lax.ppermute(part.reshape(rows), 'tp', swap)
        step = 800
        d_weight, d_bias = pl.pallas_call(
            weight_kernel,
            grid=(vocab // step,),
            out_shape=(jax.ShapeDtypeStruct((vocab, hidden), BF16), jax.ShapeDtypeStruct((vocab,), F32)),
            in_specs=[
                pl.BlockSpec((step, 2 * HALF), lambda i: (i, 0)),
                pl.BlockSpec((2 * HALF, hidden), lambda i: (0, 0), pipeline_mode=pl.Buffered(1)),
                vmem,
            ],
            out_specs=(pl.BlockSpec((step, hidden), lambda i: (i, 0)), hbm),
            scratch_shapes=[dma],
            cost_estimate=pl.CostEstimate(
                flops=2 * hidden * 2 * HALF * vocab, bytes_accessed=50_000_000, transcendentals=0
            ),
            compiler_params=pltpu.CompilerParams(vmem_limit_bytes=67_043_328),
            name='dweight',
        )(gt, hb.reshape(2 * HALF, hidden), db)
        d_hidden = pl.pallas_call(
            finish_kernel,
            out_shape=jax.ShapeDtypeStruct(rows, BF16),
            name='finish',
        )(mine.reshape(rows), near, far)
        return loss[0, :1], d_weight.T, d_bias, d_hidden.reshape(docs, doc_len, hidden)

    return jax.shard_map(
        local_step,
        mesh=mesh,
        in_specs=(row_spec, row_spec, row_spec, row_spec, P('tp'), P(None, 'tp'), P('tp')),
        out_specs=(P('dp'), P('dp', 'tp'), row_spec, row_spec),
        check_vma=False,
    )
```

```python
import functools

import jax
import jax.numpy as jnp
from jax import lax
from jax.experimental import pallas as pl
from jax.experimental.pallas import tpu as pltpu
from jax.sharding import PartitionSpec as P

REG_COEF = 32.0
MESH = pl.DeviceIdType.MESH
F32 = jnp.float32
BF16 = jnp.bfloat16
VT = 512
LANES = 128
HALF = 256
ROWS = 128
SUB = 64
CHUNKS = 4
EARLY = 256
MM_ROWS = 256
MM_COLS = 512
QUERIES = 32
NT_DIMS = (((1,), (1,)), ((), ()))
TN_DIMS = (((0,), (0,)), ((), ()))


def dot(a, b):
    return jnp.dot(a, b, preferred_element_type=F32)


def dot_nt(a, b):
    return lax.dot_general(a, b, NT_DIMS, preferred_element_type=F32)


def dot_tn(a, b):
    return lax.dot_general(a, b, TN_DIMS, preferred_element_type=F32)


def iota(shape, axis):
    return lax.broadcasted_iota(jnp.int32, shape, axis)


def one_hot(cond):
    return jnp.where(cond, 1.0, 0.0).astype(BF16)


def split3(x):
    hi = x.astype(BF16)
    rest = x - hi.astype(F32)
    mid = rest.astype(BF16)
    low = (rest - mid.astype(F32)).astype(BF16)
    return hi, mid, low


def log1p_pos(y):
    return jnp.where(y < 5e-4, y * (1.0 - 0.5 * y), jnp.log(1.0 + y))


def weave(first, second):
    count = max(len(first), 1)
    done = 0
    for k in range(count):
        if first:
            first[k]()
        upto = -(-len(second) * (k + 1) // count)
        for piece in second[done:upto]:
            piece()
        done = upto


def head_kernel(
    reg_weight,
    hid_ref, ids_ref, mask_ref, pos_ref, qw_hbm, bias_hbm, w_hbm,
    loss_ref, db_ref, gt_hbm, hb_hbm, send_hbm, mine_hbm, part_hbm,
    wv, ybuf, hb, land, raw_a, raw_b, g_a, g_b, acc1, acc2, recv1,
    counts, bm, qw_ref, bias_ref, mask_row, ids_all, mask_all, pos_all, s_acc, reg_acc, inbox, ds6,
    w_sem, hid_send, hid_recv, fwd_send, fwd_recv, pk_send, pk_recv, s_send, s_recv, acc_send, acc_recv, far_send, far_recv, free_sem, out_sem, g_sem,
):
    vocab = wv.shape[0]
    hidden = wv.shape[1]
    full = vocab // VT
    tail = vocab - full * VT
    me = lax.axis_index("tp")
    partner = me + 1 - 2 * lax.rem(me, 2)
    other = lax.rem(me + 2, 4)
    diag = lax.rem(partner + 2, 4)
    slots = (me, partner, other, diag)

    def remote(src, dst, ssem, rsem, dev):
        return pltpu.make_async_remote_copy(src, dst, ssem, rsem, device_id={"tp": dev}, device_id_type=MESH)

    def at(t, off=0, size=VT):
        if isinstance(t, int):
            return pl.ds(t * VT + off, size)
        return pl.ds(pl.multiple_of(t * VT + off, SUB), size)

    def cols(t, off=0, size=VT):
        if isinstance(t, int):
            return pl.ds(t * VT + off, size)
        return pl.ds(pl.multiple_of(t * VT + off, LANES), size)

    def w_copy(t, size=VT):
        return pltpu.make_async_copy(w_hbm.at[at(t, 0, size)], wv.at[at(t, 0, size)], w_sem.at[t])

    rows_in = [
        pltpu.make_async_copy(qw_hbm, qw_ref.at[0], out_sem.at[0]),
        pltpu.make_async_copy(bias_hbm, bias_ref.at[0], out_sem.at[1]),
    ]
    for c in rows_in:
        c.start()
    ahead = 4
    for t in range(ahead):
        w_copy(t).start()

    barrier = pltpu.get_barrier_semaphore()
    for peer in slots[1:]:
        pl.semaphore_signal(barrier, inc=1, device_id={"tp": peer}, device_id_type=MESH)
    pl.semaphore_wait(barrier, 3)

    pk_copies = []
    for k in range(3):
        for i, (src, dst) in enumerate(((ids_ref, ids_all), (mask_ref, mask_all), (pos_ref, pos_all))):
            pk_copies.append(remote(src, dst.at[me], pk_send.at[3 * k + i], pk_recv.at[3 * k + i], slots[k + 1]))
    for c in pk_copies:
        c.start()
    near = remote(hid_ref, land.at[0], hid_send.at[CHUNKS], hid_recv.at[CHUNKS], partner)
    near.start()
    step = ROWS // CHUNKS
    far, relay = [], []
    for k in range(CHUNKS):
        part = pl.ds(k * step, step)
        far.append(remote(hid_ref.at[part], land.at[1, part], hid_send.at[k], hid_recv.at[k], other))
        relay.append(remote(land.at[1, part], land.at[2, part], fwd_send.at[k], fwd_recv.at[k], partner))
    for c in far:
        c.start()

    ones = jnp.ones((16, LANES), BF16)
    sub16 = iota((16, VT), 0)

    def bias_columns(t, size):
        parts = [p.astype(F32) for p in split3(bias_ref[:, cols(t, 0, size)])]
        stack = jnp.zeros((16, size), F32)
        for k in range(3):
            stack = jnp.where(sub16[:, :size] == k, parts[k], stack)
        bm[at(t, 0, size)] = dot_tn(stack.astype(BF16), ones)

    def bias_piece(t, size=VT):
        return [functools.partial(bias_columns, t, size)]

    ids_all[me] = ids_ref[...]
    mask_all[me] = mask_ref[...]
    pos_all[me] = pos_ref[...]
    for c in pk_copies:
        c.wait_recv()

    lane8 = iota((8, LANES), 1)
    for h in range(2):
        total = None
        for k in range(2):
            mask = mask_all[slots[2 * h + k]].astype(F32).astype(BF16)
            spread = dot(mask, one_hot((iota((16, LANES), 1) >> 4) + 8 == iota((16, LANES), 0)))
            piece = jnp.sum(jnp.where((lane8 & 15) == iota((8, LANES), 0) + 8 * k, spread, 0.0), axis=0, keepdims=True)
            total = piece if total is None else total + piece
        mask_row[h] = jnp.broadcast_to(total, (8, LANES))

    ids = jnp.concatenate([ids_all[g] for g in range(4)], axis=0)
    raw_a[pl.ds(0, LANES), pl.ds(0, LANES)] = jnp.zeros((LANES, LANES), F32)
    raw_a[pl.ds(0, QUERIES), pl.ds(0, 64)] = ids.astype(F32)
    ids_t = jnp.transpose(raw_a[pl.ds(0, LANES), pl.ds(0, LANES)])
    high = (ids - me * vocab) >> 7
    low = (ids_t.astype(jnp.int32) - me * vocab) & 127
    for q in range(QUERIES):
        hot_hi = one_hot(iota((64, 64), 0) == high[q:q + 1])
        hot_lo = one_hot(iota((64, LANES), 1) == low[:64, q:q + 1])
        counts[pl.ds(q, 64, QUERIES), :] = dot(hot_hi, hot_lo)
    s_acc[...] = jnp.zeros_like(s_acc)
    reg_acc[...] = jnp.zeros_like(reg_acc)

    def place(half, sources):
        r, k = iota((HALF, ROWS), 0), iota((HALF, ROWS), 1)
        pick = [one_hot((k == (r & 7) * 16 + (r >> 4)) & (((r >> 3) & 1) == s)) for s in range(2)]
        for c in range(hidden // VT):
            block = pl.ds(c * VT, VT)
            mixed = dot(pick[0], sources[0][:, block]) + dot(pick[1], sources[1][:, block])
            hb[half, :, block] = mixed.astype(BF16)

    for c in rows_in:
        c.wait()
    bias_columns(0, VT)
    near.wait_recv()
    place(0, (hid_ref, land.at[0]))

    def query_rep(t, off, size):
        out = []
        for c in range(-(-size // LANES)):
            width = min(LANES, size - c * LANES)
            block = t * (VT // LANES) + off // LANES + c
            start = block * QUERIES
            if not isinstance(t, int):
                start = pl.multiple_of(start, QUERIES)
            cnt = counts[pl.ds(start, QUERIES)]
            out.append(cnt[:, :width] * qw_ref[:, cols(t, off + c * LANES, width)])
        return jnp.concatenate(out, axis=1) if len(out) > 1 else out[0]

    def mm(t, half, buf, size=VT):
        def piece(off, depth):
            def run():
                buf[pl.ds(off, depth)] = dot_nt(wv[at(t, off, depth)], hb[half])
            return run
        return [piece(off, min(MM_ROWS, size - off)) for off in range(0, size, MM_ROWS)]

    lane_sub = iota((SUB, LANES), 1)

    def ep(t, half, buf, size=VT):
        def rows_piece(r):
            def run():
                mask = mask_row[half, 0:1]
                rows = pl.ds(r * SUB, SUB)
                here = at(t, r * SUB, SUB)
                col = bm[here]
                bias = col if half == 0 else jnp.broadcast_to(col[:, 0:1], (SUB, LANES))
                acc = None
                for b in range(2):
                    y = jnp.maximum(buf[rows, pl.ds(b * LANES, LANES)] + bias, 0.0)
                    if b == 1:
                        y = y * mask
                    ybuf[here, pl.ds(half * HALF + b * LANES, LANES)] = y
                    act = log1p_pos(y)
                    acc = act if acc is None else acc + act
                buf[rows, pl.ds(0, LANES)] = acc
                total = jnp.sum(acc, axis=1, keepdims=True)
                if half == 0:
                    bm[here] = jnp.where(lane_sub < 64, col, total)
                else:
                    mean = jnp.broadcast_to((total + col[:, 64:65]) * (1.0 / 32.0), (SUB, LANES))
                    bm[here] = mean
                    square = mean * mean
                    reg_acc[...] += jnp.sum(square.reshape(SUB // 8, 8, LANES), axis=0)
            return run

        def score_piece(off):
            def run():
                depth = min(HALF, size - off)
                rq = split3(query_rep(t, off, depth))
                act = split3(buf[pl.ds(off, depth), pl.ds(0, LANES)])
                s_acc[half] += dot(jnp.concatenate(rq, axis=0), act[0])
                s_acc[half, pl.ds(0, 64)] += dot(jnp.concatenate(rq[:2], axis=0), act[1])
                s_acc[half, pl.ds(0, 32)] += dot(rq[0], act[2])
            return run

        out = []
        for off in range(0, size, HALF):
            for r in range(off // SUB, min(off + HALF, size) // SUB):
                out.append(rows_piece(r))
            out.append(score_piece(off))
        return out

    def forward(half, tick):
        first = half == 0
        if first:
            w_copy(0).wait()
        weave(mm(0, half, raw_a), [])

        def body(i, carry):
            t = 2 * i
            if first:
                for u in range(2):
                    @pl.when(t + u + ahead < full)
                    def _():
                        w_copy(t + u + ahead).start()
                @pl.when(i == (full - ahead) // 2)
                def _():
                    w_copy(full, tail).start()
                w_copy(t + 1).wait()
            weave(mm(t + 1, half, raw_b), (bias_piece(t + 1) if first else []) + ep(t, half, raw_a))
            if first:
                w_copy(t + 2).wait()
            weave(mm(t + 2, half, raw_a), (bias_piece(t + 2) if first else []) + ep(t + 1, half, raw_b))
            tick(i)
            return carry

        lax.fori_loop(0, (full - 1) // 2, body, 0)
        if first:
            w_copy(full, tail).wait()
        weave(mm(full, half, raw_b, tail), (bias_piece(full, tail) if first else []) + ep(full - 1, half, raw_a))
        weave([], ep(full, half, raw_b, tail))

    def relay_tick(i):
        for k, when in enumerate((0, 2, 4)):
            @pl.when(i == when)
            def _():
                far[k].wait_recv()
                relay[k].start()

    forward(0, relay_tick)
    far[CHUNKS - 1].wait_recv()
    relay[CHUNKS - 1].start()
    for c in relay:
        c.wait_recv()
    place(1, (land.at[1], land.at[2]))
    hb_out = pltpu.make_async_copy(hb, hb_hbm, out_sem.at[3])
    hb_out.start()
    forward(1, lambda i: None)

    def doc_lane(half):
        k = iota((LANES, LANES), 0)
        owner = jnp.where(((k >> 3) & 1) == 0, slots[2 * half], slots[2 * half + 1])
        return one_hot(iota((LANES, LANES), 1) == owner * 8 + (k & 7))

    scores = None
    for h in range(2):
        mine = s_acc[h, pl.ds(0, 32)] + s_acc[h, pl.ds(32, 32)] + s_acc[h, pl.ds(64, 32)]
        moved = dot(jnp.concatenate(split3(mine), axis=0), doc_lane(h))
        moved = moved[0:32] + moved[32:64] + moved[64:96]
        scores = moved if scores is None else scores + moved
    inbox[me, pl.ds(0, 32)] = scores
    inbox[me, pl.ds(32, 8)] = jnp.broadcast_to(jnp.sum(reg_acc[...], axis=0, keepdims=True), (8, LANES))
    s_copies = [remote(inbox.at[me], inbox.at[me], s_send.at[k], s_recv.at[k], slots[k + 1]) for k in range(3)]
    for c in s_copies:
        c.start()
    for c in s_copies:
        c.wait_recv()
    st = inbox[0] + inbox[1] + inbox[2] + inbox[3]
    lane = iota((32, LANES), 1)
    live = lane < 32
    score = jnp.where(live, st[0:32], -3.0e38)
    diagonal = iota((8, 8), 0) == iota((8, 8), 1)
    pos = jnp.concatenate(
        [jnp.sum(jnp.where(diagonal, pos_all[g].astype(F32), 0.0), axis=1, keepdims=True) for g in range(4)], axis=0
    ).astype(jnp.int32)
    onehot = jnp.where(lane == pos, 1.0, 0.0)
    top = jnp.max(score, axis=1, keepdims=True)
    expo = jnp.where(live, jnp.exp(score - top), 0.0)
    norm = jnp.sum(expo, axis=1, keepdims=True)
    per_query = top + jnp.log(norm) - jnp.sum(jnp.where(live, score, 0.0) * onehot, axis=1, keepdims=True)
    loss = jnp.sum(per_query, axis=0, keepdims=True) * (1.0 / 32.0) + st[32:33] * reg_weight
    loss_ref[...] = loss
    d_scores = split3(jnp.where(live, expo / norm - onehot, 0.0) * (1.0 / 32.0))
    for b, h in enumerate((1, 0)):
        lanes = [dot_nt(p, doc_lane(h)).astype(BF16) for p in d_scores]
        for k, p in enumerate((0, 1, 0, 2, 1, 0)):
            ds6[pl.ds(k * 32, 32), pl.ds(b * LANES, LANES)] = lanes[p]

    def g_copy(t, half, buf, k, size=VT):
        return pltpu.make_async_copy(
            buf.at[pl.ds(0, size)], gt_hbm.at[at(t, 0, size), pl.ds(half * HALF, HALF)], g_sem.at[k]
        )

    def setup(t, half, size=VT):
        def piece(off):
            def run():
                depth = min(HALF, size - off)
                hi, mid, lo = split3(query_rep(t, off, depth))
                raw_a[pl.ds(off, depth)] = dot_tn(jnp.concatenate([hi, hi, mid, hi, mid, lo], axis=0), ds6[...])
            return run
        return [piece(off) for off in range(0, size, HALF)] if half == 1 else []

    def grad(t, half, buf, k, size=VT):
        def rows_piece(r):
            def run():
                rows = pl.ds(r * SUB, SUB)
                here = at(t, r * SUB, SUB)
                d_rep = bm[here]
                if half == 1:
                    reg = d_rep * (2.0 * reg_weight / 32.0)
                    d_rep = raw_a[rows, pl.ds(0, LANES)] + reg
                    bm[here] = raw_a[rows, pl.ds(LANES, LANES)] + reg
                total = None
                for b in range(2):
                    y = ybuf[here, pl.ds(half * HALF + b * LANES, LANES)]
                    d = jnp.where(y > 0.0, d_rep * (1.0 / (1.0 + y)), 0.0)
                    total = d if total is None else total + d
                    buf[rows, pl.ds(b * LANES, LANES)] = d.astype(BF16)
                raw_b[rows, pl.ds(0, LANES)] = total
            return run

        def finish():
            g_copy(t, half, buf, k, size).start()
            for off in range(0, size, LANES):
                width = min(LANES, size - off)
                row = jnp.sum(jnp.transpose(raw_b[pl.ds(off, LANES), pl.ds(0, LANES)]), axis=0, keepdims=True)[:, :width]
                if half == 1:
                    db_ref[:, cols(t, off, width)] = row
                else:
                    db_ref[:, cols(t, off, width)] += row

        return [rows_piece(r) for r in range(size // SUB)] + [finish]

    def mm_t(t, buf, acc, size=VT):
        def piece(n):
            def run():
                block = pl.ds(n * MM_COLS, MM_COLS)
                acc[:, :, block] += dot_tn(buf[pl.ds(0, size)], wv[at(t, 0, size), block]).reshape(16, 16, MM_COLS)
            return run
        return [piece(n) for n in range(hidden // MM_COLS)]

    def backward(half, acc, tick):
        acc[...] = jnp.zeros_like(acc)
        weave([], setup(0, half) + grad(0, half, g_a, 0) + setup(1, half))

        def setup_next(t):
            return setup(jnp.minimum(t, full - 1), half)

        def body(i, carry):
            t = 2 * i

            @pl.when(i > 0)
            def _():
                g_copy(t - 1, half, g_b, 1).wait()
            weave(mm_t(t, g_a, acc), grad(t + 1, half, g_b, 1) + setup(t + 2, half))
            g_copy(t, half, g_a, 0).wait()
            weave(mm_t(t + 1, g_b, acc), grad(t + 2, half, g_a, 0) + setup_next(t + 3))
            tick(i)
            return carry

        lax.fori_loop(0, (full - 1) // 2, body, 0)
        g_copy(full - 2, half, g_b, 1).wait()
        weave(mm_t(full - 1, g_a, acc), setup(full, half, tail) + grad(full, half, g_b, 1, tail))
        weave(mm_t(full, g_b, acc, tail), [])
        g_copy(full - 1, half, g_a, 0).wait()
        g_copy(full, half, g_b, 1, tail).wait()

    backward(1, acc1, lambda i: None)
    swap = remote(acc1.at[:, pl.ds(8, 8)], recv1, acc_send, acc_recv, partner)
    swap.start()
    outs = [
        pltpu.make_async_copy(acc1.at[:, pl.ds(0, 8), pl.ds(EARLY, hidden - EARLY)], send_hbm, out_sem.at[0]),
        pltpu.make_async_copy(acc2.at[:, pl.ds(0, 8)], mine_hbm, out_sem.at[1]),
        pltpu.make_async_copy(acc2.at[:, pl.ds(8, 8)], part_hbm, out_sem.at[2]),
    ]

    early = remote(acc1.at[:, pl.ds(0, 8), pl.ds(0, EARLY)], recv1.at[:, :, pl.ds(0, EARLY)], far_send, far_recv, other)

    def swap_tick(i):
        @pl.when(i == 1)
        def _():
            swap.wait_recv()
            acc1[:, pl.ds(0, 8)] += recv1[...]
            outs[0].start()
            pl.semaphore_signal(free_sem, inc=1, device_id={"tp": other}, device_id_type=MESH)

        @pl.when(i == 2)
        def _():
            pl.semaphore_wait(free_sem, 1)
            early.start()

    backward(0, acc2, swap_tick)
    outs[2].start()
    early.wait_recv()
    acc2[:, pl.ds(0, 8), pl.ds(0, EARLY)] += recv1[:, :, pl.ds(0, EARLY)]
    outs[1].start()
    for c in outs:
        c.wait()
    hb_out.wait()
    swap.wait_send()
    early.wait_send()
    near.wait_send()
    for c in pk_copies + far + relay + s_copies:
        c.wait_send()


def weight_kernel(gt_ref, hb_ref, db_ref, out_ref, db_hbm, sem):
    copy = pltpu.make_async_copy(db_ref.at[0], db_hbm, sem)
    pl.when(pl.program_id(0) == 0)(copy.start)
    pl.when(pl.program_id(0) == pl.num_programs(0) - 1)(copy.wait)
    out_ref[...] = dot(gt_ref[...], hb_ref[...]).astype(BF16)


def finish_kernel(mine_ref, part_ref, far_ref, out_ref):
    r, k = iota((ROWS, ROWS), 0), iota((ROWS, ROWS), 1)
    perm = one_hot(k == (r & 15) * 8 + (r >> 4))
    total = mine_ref[...] + part_ref[...]
    early, late = pl.ds(0, EARLY), pl.ds(EARLY, total.shape[1] - EARLY)
    out_ref[:, early] = dot(perm, total[:, :EARLY].astype(BF16)).astype(BF16)
    out_ref[:, late] = dot(perm, (total[:, EARLY:] + far_ref[...]).astype(BF16)).astype(BF16)


def solution(mesh):
    group_size = mesh.shape['tp']
    row_spec = P(('dp', 'tp'))

    def local_step(doc_hidden, doc_mask, query_ids, positive, tok_weight, w_head, b_head):
        docs, doc_len, hidden = doc_hidden.shape
        vocab = w_head.shape[1]
        reg_weight = REG_COEF / (vocab * group_size * doc_len * doc_len)
        tiles = -(-vocab // VT)
        vmem = pl.BlockSpec(memory_space=pltpu.VMEM)
        hbm = pl.BlockSpec(memory_space=pl.ANY)
        dma = pltpu.SemaphoreType.DMA
        block = jax.ShapeDtypeStruct((16, 8, hidden), F32)
        loss, db, gt, hb, send, mine, part = pl.pallas_call(
            functools.partial(head_kernel, reg_weight),
            out_shape=(
                jax.ShapeDtypeStruct((1, LANES), F32),
                jax.ShapeDtypeStruct((1, vocab), F32),
                jax.ShapeDtypeStruct((vocab, 2 * HALF), BF16),
                jax.ShapeDtypeStruct((2, HALF, hidden), BF16),
                jax.ShapeDtypeStruct((16, 8, hidden - EARLY), F32), block, block,
            ),
            in_specs=[vmem, vmem, vmem, vmem, hbm, hbm, hbm],
            out_specs=(vmem, vmem, hbm, hbm, hbm, hbm, hbm),
            scratch_shapes=[
                pltpu.VMEM((vocab, hidden), BF16),
                pltpu.VMEM((vocab, 2 * HALF), F32),
                pltpu.VMEM((2, HALF, hidden), BF16),
                pltpu.VMEM((3, ROWS, hidden), BF16),
                pltpu.VMEM((VT, HALF), F32),
                pltpu.VMEM((VT, HALF), F32),
                pltpu.VMEM((VT, HALF), BF16),
                pltpu.VMEM((VT, HALF), BF16),
                pltpu.VMEM((16, 16, hidden), F32),
                pltpu.VMEM((16, 16, hidden), F32),
                pltpu.VMEM((16, 8, hidden), F32),
                pltpu.VMEM((64 * QUERIES, LANES), F32),
                pltpu.VMEM((vocab, LANES), F32),
                pltpu.VMEM((1, vocab), F32),
                pltpu.VMEM((1, vocab), F32),
                pltpu.VMEM((2, 8, LANES), F32),
                pltpu.VMEM((4, 8, 64), jnp.int32),
                pltpu.VMEM((4, 8, 16), jnp.int32),
                pltpu.VMEM((4, 1, 8), jnp.int32),
                pltpu.VMEM((2, 96, LANES), F32),
                pltpu.VMEM((8, LANES), F32),
                pltpu.VMEM((4, 40, LANES), F32),
                pltpu.VMEM((192, HALF), BF16),
                dma((tiles,)), dma((CHUNKS + 1,)), dma((CHUNKS + 1,)), dma((CHUNKS,)), dma((CHUNKS,)),
                dma((9,)), dma((9,)), dma((3,)), dma((3,)), dma, dma, dma, dma, pltpu.SemaphoreType.REGULAR, dma((5,)), dma((2,)),
            ],
            compiler_params=pltpu.CompilerParams(
                collective_id=0, has_side_effects=True, vmem_limit_bytes=67_043_328
            ),
            name='head',
        )(
            doc_hidden.reshape(docs * doc_len, hidden), query_ids, doc_mask, positive.reshape(1, 8),
            tok_weight, b_head, w_head.T,
        )

        cross = [(k, (k + 2) % 4) for k in range(4)]
        swap = [(k, k ^ 1) for k in range(4)]
        rows = (docs * doc_len, hidden)
        far = lax.ppermute(send.reshape(rows[0], hidden - EARLY), 'tp', cross)
        near = lax.ppermute(part.reshape(rows), 'tp', swap)
        step = 800
        d_weight, d_bias = pl.pallas_call(
            weight_kernel,
            grid=(vocab // step,),
            out_shape=(jax.ShapeDtypeStruct((vocab, hidden), BF16), jax.ShapeDtypeStruct((vocab,), F32)),
            in_specs=[
                pl.BlockSpec((step, 2 * HALF), lambda i: (i, 0)),
                pl.BlockSpec((2 * HALF, hidden), lambda i: (0, 0), pipeline_mode=pl.Buffered(1)),
                vmem,
            ],
            out_specs=(pl.BlockSpec((step, hidden), lambda i: (i, 0)), hbm),
            scratch_shapes=[dma],
            cost_estimate=pl.CostEstimate(
                flops=2 * hidden * 2 * HALF * vocab, bytes_accessed=50_000_000, transcendentals=0
            ),
            compiler_params=pltpu.CompilerParams(vmem_limit_bytes=67_043_328),
            name='dweight',
        )(gt, hb.reshape(2 * HALF, hidden), db)
        d_hidden = pl.pallas_call(
            finish_kernel,
            out_shape=jax.ShapeDtypeStruct(rows, BF16),
            name='finish',
        )(mine.reshape(rows), near, far)
        return loss[0, :1], d_weight.T, d_bias, d_hidden.reshape(docs, doc_len, hidden)

    return jax.shard_map(
        local_step,
        mesh=mesh,
        in_specs=(row_spec, row_spec, row_spec, row_spec, P('tp'), P(None, 'tp'), P('tp')),
        out_specs=(P('dp'), P('dp', 'tp'), row_spec, row_spec),
        check_vma=False,
    )
```
